512 devices in a mesh: ka: 64 (over y, z_hi, x, core), col: 8 (over z_lo).
Axes of the slice: x: 4, y: 4, z: 16 (z_hi: 2, z_lo: 8; z = z_hi * 8 + z_lo), core: 2. Of those that a mesh axis runs over, the one named last changes fastest.
Arguments:
- correlations: bfloat16 [64, 8, 2, 512, 512], P('ka', None, None, 'col')
- gauge: bfloat16 [64, 512, 2, 256], P('ka', 'col'), may hold values from -1 to 1
- neighbours: int32 [64, 8], P('ka'), may hold values from 0 to 63, as said below
- shifts: int32 [64, 8, 3], P('ka'), may hold values from -1 to 1, as said below
Outputs:
- u_next: float32 [64, 512, 2, 256], P('ka', 'col')
- gradient: float32 [64, 2, 256, 256], P('ka', None, 'col')
- omega_od: float32 [], replicated
The draws below stay inside these ranges and needn't reach their ends.
Inputs may be any that keep to these rules, and one draw needn't show every extreme that they name: For each k-point k with grid coordinates g(k) = (k // 16, k // 4 % 4, k % 4) on the 4 x 4 x 4 grid, the 8 entries neighbours[k, :] together with shifts[k, :, :] list the displacements d = +-(1,0,0), +-(0,1,0), +-(0,0,1), +-(1,1,1), each once, in some order: g(neighbours[k,b]) = g(k) + d - shifts[k,b] * (4, 4, 4), with each coordinate inside the grid. shifts[k,b] is the componentwise floor of (g(k) + d) / (4, 4, 4) for the displacement d that neighbours[k,b] names.
All inputs are finite; a program needn't handle non-finite values.
Results may differ from the reference program's by a relative error of at most 0.02.
Values may be sent and summed in bfloat16 or wider, within the bound.
No kernel may reach another device: no remote copies, remote signals or barrier semaphores. Data moves between devices by JAX's collectives and lax.ppermute only.
A program may use at most 128 MiB of HBM per device.

```python
import jax
import jax.numpy as jnp
from jax import lax

NB = 512
NW = 256
NBV = 8
NS_STEPS = 3
KPOINT_COUNT = 64
NK1 = 4
NBLK = 8


def shell_table():
    return jnp.array([[1, 0, 0], [-1, 0, 0], [0, 1, 0], [0, -1, 0], [0, 0, 1], [0, 0, -1], [1, 1, 1], [-1, -1, -1]], jnp.int32)


def neighbour_table(key):
    sub = jax.random.fold_in(key, 7)
    keys = jax.random.split(sub, KPOINT_COUNT)
    order = jax.vmap(lambda single: jax.random.permutation(single, NBV))(keys)
    displacement = shell_table()[order]
    kpoint_index = jnp.arange(KPOINT_COUNT, dtype=jnp.int32)
    lattice_positions = jnp.stack([kpoint_index // 16, kpoint_index // 4 % 4, kpoint_index % 4], -1)
    grid_sizes = jnp.array([NK1, 4, 4], jnp.int32)
    target = lattice_positions[:, None, :] + displacement
    wraps = jnp.floor_divide(target, grid_sizes)
    inside = target - wraps * grid_sizes
    index = inside[..., 0] * 16 + inside[..., 1] * 4 + inside[..., 2]
    return (index.astype(jnp.int32), wraps.astype(jnp.int32))


def draw_neighbours(key, part):
    return neighbour_table(key)[0]


def draw_shifts(key, part):
    return neighbour_table(key)[1]


def draw_gauge(key, part):
    first, second = jax.random.split(jax.random.fold_in(key, 17))
    shape = (KPOINT_COUNT, NB, NW)
    real = jax.random.normal(first, shape, jnp.float32)
    imag = jax.random.normal(second, shape, jnp.float32)
    factor = 1.0 / (jnp.sqrt(2.0 * NB) * 1.1 * (1.0 + jnp.sqrt(NW / NB)))
    real, imag = (real * factor, imag * factor)
    high = lax.Precision.HIGHEST
    eye = jnp.eye(NW, dtype=jnp.float32)
    for turn in range(16):
        gram_r = jnp.einsum('krm,krn->kmn', real, real, precision=high) + jnp.einsum('krm,krn->kmn', imag, imag, precision=high)
        gram_i = jnp.einsum('krm,krn->kmn', real, imag, precision=high) - jnp.einsum('krm,krn->kmn', imag, real, precision=high)
        mult_r = (3.0 * eye - gram_r) / 2.0
        mult_i = -gram_i / 2.0
        new_r = jnp.einsum('krm,kmn->krn', real, mult_r, precision=high) - jnp.einsum('krm,kmn->krn', imag, mult_i, precision=high)
        new_i = jnp.einsum('krm,kmn->krn', real, mult_i, precision=high) + jnp.einsum('krm,kmn->krn', imag, mult_r, precision=high)
        real, imag = (new_r, new_i)
    return jnp.clip(jnp.stack([real, imag], 2), -1.0, 1.0).astype(jnp.bfloat16)


def draw_correlations(key, part):
    ramp = 1.0 + 2.0 * jnp.arange(KPOINT_COUNT, dtype=jnp.float32) / (KPOINT_COUNT - 1)
    scale = jnp.sqrt(ramp / NB).reshape(KPOINT_COUNT, 1, 1, 1, 1)
    shape = (KPOINT_COUNT, NBV, 2, NB, NB)
    values = jax.random.normal(jax.random.fold_in(key, 13), shape, jnp.float32)
    return (values * scale).astype(jnp.bfloat16)


def setup_inputs(seed: int = 0) -> dict:
    streams_of = jax.random.split(jax.random.key(seed), 5)
    return {
        "correlations": draw_correlations(jax.random.fold_in(streams_of[4], 71), 0),
        "gauge": draw_gauge(jax.random.fold_in(streams_of[4], 71), 0),
        "neighbours": draw_neighbours(jax.random.fold_in(streams_of[4], 71), 0),
        "shifts": draw_shifts(jax.random.fold_in(streams_of[4], 71), 0),
    }


HIGH = lax.Precision.HIGHEST
MIXING = 0.02
STEP_LENGTH = 0.2

def grid_positions(index):
    return jnp.stack([index // 16, index // 4 % 4, index % 4], -1)

def shell_vector_weights(kpoint_index, neighbour_list, shifts):
    grid_sizes = jnp.array([NK1, 4, 4], jnp.float32)
    fractional_position = (grid_positions(neighbour_list) - grid_positions(kpoint_index)[..., None, :]).astype(jnp.float32) / grid_sizes
    fractional_position = fractional_position + shifts.astype(jnp.float32)
    cart_x = -fractional_position[..., 0] + fractional_position[..., 1] + fractional_position[..., 2]
    cart_y = fractional_position[..., 0] - fractional_position[..., 1] + fractional_position[..., 2]
    cart_z = fractional_position[..., 0] + fractional_position[..., 1] - fractional_position[..., 2]
    return 3.0 / (NBV * (cart_x * cart_x + cart_y * cart_y + cart_z * cart_z))

def cprod(form, ar, ai, br, bi, conj_left, conj_right):
    ar, ai, br, bi = [v.astype(jnp.float32) for v in (ar, ai, br, bi)]
    sign_a = -1.0 if conj_left else 1.0
    sign_b = -1.0 if conj_right else 1.0
    e = lambda p, q: jnp.einsum(form, p, q, precision=HIGH)
    real = e(ar, br) - sign_a * sign_b * e(ai, bi)
    imag = sign_b * e(ar, bi) + sign_a * e(ai, br)
    return (real, imag)

def one_point(items):
    mats, own, near, shell_weights = items
    bf = jnp.bfloat16
    qr, qi = cprod('rw,bcr->bwc', own[:, 0], own[:, 1], mats[:, 0], mats[:, 1], True, False)
    qr, qi = (qr.astype(bf), qi.astype(bf))
    blocks = NB // NBLK
    qbr = qr.reshape(NBV, NW, NBLK, blocks)
    qbi = qi.reshape(NBV, NW, NBLK, blocks)
    nbr_r = near[:, :, 0].reshape(NBV, NBLK, blocks, NW)
    nbr_i = near[:, :, 1].reshape(NBV, NBLK, blocks, NW)
    pr, pi = cprod('bwgc,bgcn->bgwn', qbr, qbi, nbr_r, nbr_i, False, False)
    mtr = lax.optimization_barrier(jnp.sum(pr.astype(bf).astype(jnp.float32), 1)).astype(bf)
    mti = lax.optimization_barrier(jnp.sum(pi.astype(bf).astype(jnp.float32), 1)).astype(bf)
    vr, vi = cprod('brm,bnm->brn', near[:, :, 0], near[:, :, 1], mtr, mti, False, True)
    vr = (shell_weights[:, None, None] * vr).astype(bf)
    vi = (shell_weights[:, None, None] * vi).astype(bf)
    yr, yi = cprod('bji,bjn->in', mats[:, 0], mats[:, 1], vr, vi, False, False)
    mr, mi = (mtr.astype(jnp.float32), mti.astype(jnp.float32))
    wr, wi = (shell_weights[:, None, None] * mr, shell_weights[:, None, None] * mi)
    hr, hi = cprod('bmn,bkn->mk', wr, wi, mr, mi, False, True)
    diag_r = jnp.diagonal(mr, 0, 1, 2)[:, None, :]
    diag_i = jnp.diagonal(mi, 0, 1, 2)[:, None, :]
    rr = mr * diag_r + mi * diag_i
    ri = mi * diag_r - mr * diag_i
    wts = shell_weights[:, None, None]
    gr = 2.0 * lax.optimization_barrier(jnp.sum(wts * (rr - jnp.swapaxes(rr, 1, 2)), 0))
    gi = 2.0 * lax.optimization_barrier(jnp.sum(wts * (ri + jnp.swapaxes(ri, 1, 2)), 0))
    square = mr * mr + mi * mi
    offdiag = lax.optimization_barrier(jnp.sum(square, (1, 2))) - lax.optimization_barrier(jnp.sum(jnp.diagonal(square, 0, 1, 2), 1))
    omega = jnp.sum(shell_weights * offdiag) / (KPOINT_COUNT * NW)
    ur, ui = (own[:, 0].astype(jnp.float32), own[:, 1].astype(jnp.float32))
    uhr, uhi = cprod('rm,mn->rn', ur, ui, hr, hi, False, False)
    ugr, ugi = cprod('rm,mn->rn', ur, ui, gr, gi, False, False)
    xr = ur + MIXING * (yr - uhr) + STEP_LENGTH * ugr
    xi = ui + MIXING * (yi - uhi) + STEP_LENGTH * ugi
    sr, si = cprod('rm,rn->mn', xr, xi, xr, xi, True, False)
    scale = jnp.sqrt(NW / (2.0 * jnp.trace(sr)))
    xr, xi = (xr * scale, xi * scale)
    sr, si = (sr * scale * scale, si * scale * scale)
    eye = jnp.eye(NW, dtype=jnp.float32)
    for turn in range(NS_STEPS):
        xr, xi = cprod('rm,mn->rn', xr, xi, (3.0 * eye - sr) / 2.0, -si / 2.0, False, False)
        if turn + 1 < NS_STEPS:
            sr, si = cprod('rm,rn->mn', xr, xi, xr, xi, True, False)
    return (jnp.stack([xr, xi], 1), jnp.stack([gr, gi], 0), omega)

def reference(correlations, gauge, neighbours, shifts):
    kpoint_index = jnp.arange(KPOINT_COUNT, dtype=jnp.int32)
    shell_weights = shell_vector_weights(kpoint_index, neighbours, shifts)
    near = gauge[neighbours]
    u_next, gradient, omega = lax.map(one_point, (correlations, gauge, near, shell_weights))
    return (u_next, gradient, jnp.sum(omega))
```

```python
import jax
import jax.numpy as jnp
from jax import lax
from jax.experimental import pallas as pl
from jax.experimental.pallas import tpu as pltpu
from jax.sharding import PartitionSpec as P

MIXING = 0.02
STEP_LENGTH = 0.2
SHELL_LIST = [
    (1, 0, 0),
    (-1, 0, 0),
    (0, 1, 0),
    (0, -1, 0),
    (0, 0, 1),
    (0, 0, -1),
    (1, 1, 1),
    (-1, -1, -1),
]
HALVES = [[0, 1, 2, 3], [4, 5, 6, 7]]
F32 = jnp.float32
BF = jnp.bfloat16


def dot(a, b):
    return lax.dot_general(a, b, (((1,), (0,)), ((), ())), preferred_element_type=F32)


def dot_nt(a, b):
    return lax.dot_general(a, b, (((1,), (1,)), ((), ())), preferred_element_type=F32)


def grid_positions(index):
    return jnp.stack([index // 16, index // 4 % 4, index % 4], -1)


def shell_vector_weights(kpoint_index, neighbour_list, shifts):
    grid_sizes = jnp.array([4, 4, 4], F32)
    f = (grid_positions(neighbour_list) - grid_positions(kpoint_index)[..., None, :]).astype(
        F32
    ) / grid_sizes
    f = f + shifts.astype(F32)
    cx = -f[..., 0] + f[..., 1] + f[..., 2]
    cy = f[..., 0] - f[..., 1] + f[..., 2]
    cz = f[..., 0] + f[..., 1] - f[..., 2]
    return 3.0 / (len(SHELL_LIST) * (cx * cx + cy * cy + cz * cz))


def slot_of(dx, dy, dz):
    diagonal = jnp.logical_and(dx != 0, dy != 0)
    pair = jnp.where(diagonal, 3, jnp.where(dx != 0, 0, jnp.where(dy != 0, 1, 2)))
    return 2 * pair + jnp.where(dx + dy + dz < 0, 1, 0)


def sort_kernel(k_ref, near_ref, shift_ref, m_ref, out_ref, sems):
    k = k_ref[0]
    copies = []
    for b in range(8):
        q = near_ref[b]
        dx = q // 16 - k // 16 + 4 * shift_ref[b, 0]
        dy = q // 4 % 4 - k // 4 % 4 + 4 * shift_ref[b, 1]
        dz = q % 4 - k % 4 + 4 * shift_ref[b, 2]
        slot = slot_of(dx, dy, dz)
        copy = pltpu.make_async_copy(m_ref.at[b], out_ref.at[slot], sems.at[b])
        copy.start()
        copies.append(copy)
    for copy in copies:
        copy.wait()


def sorted_by_displacement(kpoint_index, near, shifts, mats):
    smem = pl.BlockSpec(memory_space=pltpu.SMEM)
    hbm = pl.BlockSpec(memory_space=pl.ANY)
    return pl.pallas_call(
        sort_kernel,
        out_shape=jax.ShapeDtypeStruct(mats.shape, mats.dtype),
        in_specs=[smem, smem, smem, hbm],
        out_specs=hbm,
        scratch_shapes=[pltpu.SemaphoreType.DMA((8,))],
        name="sort_mats",
    )(kpoint_index.reshape(1), near, shifts, mats)


def rows_in_order(ref):
    return jnp.concatenate([ref[l, h] for h in range(2) for l in range(4)], 0)


def main_kernel(w_ref, m_ref, u_ref, n_ref, z_ref, g_ref, omega_ref):
    w = w_ref[0]
    a_r = m_ref[:, 0].reshape(512, 512)
    a_i = m_ref[:, 1].reshape(512, 512)
    u = rows_in_order(u_ref)
    n = rows_in_order(n_ref)
    ut = u.T
    p = dot_nt(ut, a_r)
    q = dot_nt(ut, a_i)
    qs = jnp.concatenate([p[:256] + q[256:], q[:256] - p[256:]], 0).astype(BF)
    p = dot(qs, n)
    mt_r = (p[:256, :256] - p[256:, 256:]).astype(BF)
    mt_i = (p[:256, 256:] + p[256:, :256]).astype(BF)
    mts = jnp.concatenate([mt_r, mt_i], 0)
    p = dot_nt(mts, n[:, :256])
    q = dot_nt(mts, n[:, 256:])
    vts = (w * jnp.concatenate([p[:256] + q[256:], q[:256] - p[256:]], 0)).astype(BF)
    p = dot_nt(mts, mts)
    h_r = w * (p[:256, :256] + p[256:, 256:])
    h_i = w * (p[256:, :256] - p[:256, 256:])
    mr, mi = mt_r.astype(F32), mt_i.astype(F32)
    row = lax.broadcasted_iota(jnp.int32, (256, 256), 0)
    col = lax.broadcasted_iota(jnp.int32, (256, 256), 1)
    eye = row == col
    zero = jnp.zeros_like(mr)
    only_r, only_i = jnp.where(eye, mr, zero), jnp.where(eye, mi, zero)
    row_r, row_i = only_r.sum(0, keepdims=True), only_i.sum(0, keepdims=True)
    col_r, col_i = only_r.sum(1, keepdims=True), only_i.sum(1, keepdims=True)
    tr, ti = mr.T, mi.T
    g_r = 2.0 * w * ((mr * row_r + mi * row_i) - (tr * col_r + ti * col_i))
    g_i = 2.0 * w * ((mi * row_r - mr * row_i) + (ti * col_r - tr * col_i))
    square = jnp.where(eye, zero, mr * mr + mi * mi)
    omega = jnp.sum(jnp.sum(square, 0, keepdims=True), 1, keepdims=True)
    omega_ref[...] = jnp.broadcast_to(omega * (w / (64 * 256)), omega_ref.shape)
    for r in range(8):
        g_ref[r, 0] = g_r[32 * r : 32 * r + 32].astype(BF)
        g_ref[r, 1] = g_i[32 * r : 32 * r + 32].astype(BF)
    gt_r = -STEP_LENGTH * g_r - MIXING * h_r
    gt_i = STEP_LENGTH * g_i + MIXING * h_i
    gts = jnp.concatenate([gt_r, gt_i], 0).astype(BF)
    p = dot_nt(gts, u[:, :256])
    q = dot_nt(gts, u[:, 256:])
    zt_r = p[:256] - q[256:]
    zt_i = q[:256] + p[256:]
    p = dot(vts, a_r)
    q = dot(vts, a_i)
    zt_r = (zt_r + MIXING * (p[:256] - q[256:])).astype(BF)
    zt_i = (zt_i + MIXING * (q[:256] + p[256:])).astype(BF)
    z_r, z_i = zt_r.T, zt_i.T
    for h in range(2):
        for l in range(4):
            at = 64 * (4 * h + l)
            z_ref[l, h, :, :256] = z_r[at : at + 64]
            z_ref[l, h, :, 256:] = z_i[at : at + 64]


def main_products(w, mats, full, near):
    vmem = pl.BlockSpec(memory_space=pltpu.VMEM)
    return pl.pallas_call(
        main_kernel,
        out_shape=(
            jax.ShapeDtypeStruct((4, 2, 64, 512), BF),
            jax.ShapeDtypeStruct((8, 2, 32, 256), BF),
            jax.ShapeDtypeStruct((8, 128), F32),
        ),
        in_specs=[pl.BlockSpec(memory_space=pltpu.SMEM), vmem, vmem, vmem],
        out_specs=(vmem, vmem, vmem),
        compiler_params=pltpu.CompilerParams(vmem_limit_bytes=48 << 20),
        name="main_products",
    )(w.reshape(1), mats, full, near)


def cdot(ar, ai, br, bi):
    p = dot(
        jnp.concatenate([ar, ai], 0).astype(BF), jnp.concatenate([br, bi], 1).astype(BF)
    )
    rows, cols = ar.shape[0], br.shape[1]
    return p[:rows, :cols] - p[rows:, cols:], p[:rows, cols:] + p[rows:, :cols]


def orth_kernel(x_ref, own_ref, out_ref):
    x = x_ref[...].reshape(512, 512)
    p = dot(x.T, x)
    s_r = p[:256, :256] + p[256:, 256:]
    s_i = p[:256, 256:] - p[256:, :256]
    row = lax.broadcasted_iota(jnp.int32, (256, 256), 0)
    col = lax.broadcasted_iota(jnp.int32, (256, 256), 1)
    eye = (row == col).astype(F32)
    trace = jnp.sum(jnp.sum(s_r * eye, 0, keepdims=True), 1, keepdims=True)
    square = 256 / (2.0 * trace)
    scale = jnp.sqrt(square)
    d_r = 0.5 * (eye - square * s_r)
    d_i = -0.5 * (square * s_i)
    p_r, p_i = d_r, d_i
    for _ in range(2):
        q_r, q_i = cdot(d_r, d_i, d_r, d_i)
        c_r, c_i = cdot(q_r, q_i, d_r, d_i)
        d_r, d_i = 1.5 * q_r + c_r, 1.5 * q_i + c_i
        e_r, e_i = cdot(p_r, p_i, d_r, d_i)
        p_r, p_i = p_r + d_r + e_r, p_i + d_i + e_i
    own = own_ref[...]
    o_r, o_i = own[:, :256], own[:, 256:]
    e_r, e_i = cdot(o_r, o_i, p_r, p_i)
    out_ref[:, :256] = scale * (o_r + e_r)
    out_ref[:, 256:] = scale * (o_i + e_i)


def orthonormalized(full, own):
    vmem = pl.BlockSpec(memory_space=pltpu.VMEM)
    return pl.pallas_call(
        orth_kernel,
        out_shape=jax.ShapeDtypeStruct((64, 512), F32),
        in_specs=[vmem, vmem],
        out_specs=vmem,
        compiler_params=pltpu.CompilerParams(vmem_limit_bytes=48 << 20),
        name="orthonormalize",
    )(full, own)


def within_half(x):
    return lax.all_to_all(x, "col", 0, 0, tiled=True, axis_index_groups=HALVES)


def other_half(x):
    return lax.ppermute(x, "col", [(i, i ^ 4) for i in range(8)])


def fetch_permutation():
    pairs = []
    for k in range(64):
        for c, d in enumerate(SHELL_LIST):
            g = [(a + b) % 4 for a, b in zip((k // 16, k // 4 % 4, k % 4), d)]
            pairs.append(((g[0] * 16 + g[1] * 4 + g[2]) * 8 + c, k * 8 + c))
    return pairs


def per_device(correlations, gauge, neighbours, shifts):
    kpoint_index = lax.axis_index("ka")
    cindex = lax.axis_index("col")
    low = cindex < 4
    near, shift = neighbours[0], shifts[0]

    own = gauge[0].reshape(64, 512)
    mats = sorted_by_displacement(kpoint_index, near, shift, correlations[0])
    mats = lax.all_to_all(mats, "col", 0, 0, tiled=True)
    other = other_half(own)
    quarter = jnp.where(low, jnp.stack([own, other]), jnp.stack([other, own]))
    full = within_half(jnp.broadcast_to(quarter[None], (4, 2, 64, 512)))
    near_full = lax.ppermute(full, ("ka", "col"), fetch_permutation())

    moved = grid_positions(near) - grid_positions(kpoint_index)[None] + 4 * shift
    slots = slot_of(moved[:, 0], moved[:, 1], moved[:, 2])
    weights = shell_vector_weights(kpoint_index, near, shift)
    weight = jnp.sum(jnp.where(slots == cindex, weights, 0.0))

    z, g, omega = main_products(weight, mats, full, near_full)

    z = within_half(z).astype(F32).sum(0)
    spread = lax.all_to_all(jnp.broadcast_to(omega[:1, :1], (64, 1)), "ka", 0, 0, tiled=True)
    g = lax.all_to_all(g, "col", 0, 0, tiled=True)
    z = z + other_half(z.astype(BF)).astype(F32)
    x = quarter.astype(F32) + z
    full_x = within_half(jnp.broadcast_to(x.astype(BF)[None], (4, 2, 64, 512)))
    own_x = jnp.where(low, x[0], x[1])
    u_next = orthonormalized(full_x, own_x)

    spread = jnp.broadcast_to(spread.sum(0, keepdims=True), (8, 1))
    spread = lax.all_to_all(spread, "col", 0, 0, tiled=True).sum()
    gradient = g.astype(F32).sum(0)[None]
    return (u_next.reshape(1, 64, 2, 256), gradient, spread)


def solution(mesh):
    return jax.shard_map(
        per_device,
        mesh=mesh,
        in_specs=(
            P("ka", None, None, "col", None),
            P("ka", "col", None, None),
            P("ka", None),
            P("ka", None, None),
        ),
        out_specs=(P("ka", "col", None, None), P("ka", None, "col", None), P()),
        check_vma=False,
    )
```

```python
import jax
import jax.numpy as jnp
from jax import lax
from jax.experimental import pallas as pl
from jax.experimental.pallas import tpu as pltpu
from jax.sharding import PartitionSpec as P


MIXING = 0.02
STEP_LENGTH = 0.2
SHELL_LIST = [
    (1, 0, 0),
    (-1, 0, 0),
    (0, 1, 0),
    (0, -1, 0),
    (0, 0, 1),
    (0, 0, -1),
    (1, 1, 1),
    (-1, -1, -1),
]
HALVES = [[0, 1, 2, 3], [4, 5, 6, 7]]
F32 = jnp.float32
BF = jnp.bfloat16


def dot(a, b):
    return lax.dot_general(a, b, (((1,), (0,)), ((), ())), preferred_element_type=F32)


def dot_nt(a, b):
    return lax.dot_general(a, b, (((1,), (1,)), ((), ())), preferred_element_type=F32)


def grid_positions(index):
    return jnp.stack([index // 16, index // 4 % 4, index % 4], -1)


def shell_vector_weights(kpoint_index, neighbour_list, shifts):
    grid_sizes = jnp.array([4, 4, 4], F32)
    f = (grid_positions(neighbour_list) - grid_positions(kpoint_index)[..., None, :]).astype(
        F32
    ) / grid_sizes
    f = f + shifts.astype(F32)
    cx = -f[..., 0] + f[..., 1] + f[..., 2]
    cy = f[..., 0] - f[..., 1] + f[..., 2]
    cz = f[..., 0] + f[..., 1] - f[..., 2]
    return 3.0 / (len(SHELL_LIST) * (cx * cx + cy * cy + cz * cz))


def owner_of(k, dx, dy, dz):
    diagonal = jnp.logical_and(dx != 0, dy != 0)
    plus = dx + dy + dz == jnp.where(diagonal, 3, 1)
    crosses = plus == ((k // 4) % 2 == 1)
    minus = jnp.where(plus, 0, 1)
    return jnp.where(
        diagonal,
        jnp.where(crosses, 7, 6),
        jnp.where(
            dy != 0,
            jnp.where(crosses, 0, 1),
            jnp.where(dx != 0, 2 + minus, 4 + minus),
        ),
    )


def difference(near, k):
    return (
        (near // 16 - k // 16 + 4) % 4,
        (near // 4 % 4 - k // 4 % 4 + 4) % 4,
        (near % 4 - k % 4 + 4) % 4,
    )


def fetch_permutation():
    pairs = []
    for k in range(64):
        for d in SHELL_LIST:
            g = [(a + b) % 4 for a, b in zip((k // 16, k // 4 % 4, k % 4), d)]
            plus = sum(d) > 0
            crosses = d[1] != 0 and plus == (k // 4 % 2 == 1)
            if d[0] and d[1]:
                c = 7 if crosses else 6
            elif d[1]:
                c = 0 if crosses else 1
            else:
                c = (2 if d[0] else 4) + (0 if plus else 1)
            source = 7 - c if crosses else c
            pairs.append(((g[0] * 16 + g[1] * 4 + g[2]) * 8 + source, k * 8 + c))
    return pairs


def sort_kernel(k_ref, near_ref, m_ref, out_ref, sems):
    k = k_ref[0]
    copies = []
    for b in range(8):
        slot = owner_of(k, *difference(near_ref[b], k))
        copy = pltpu.make_async_copy(m_ref.at[b], out_ref.at[slot], sems.at[b])
        copy.start()
        copies.append(copy)
    for copy in copies:
        copy.wait()


def sorted_by_owner(kpoint_index, near, mats):
    smem = pl.BlockSpec(memory_space=pltpu.SMEM)
    return pl.pallas_call(
        sort_kernel,
        out_shape=jax.ShapeDtypeStruct(mats.shape, mats.dtype),
        in_specs=[smem, smem, pl.BlockSpec(memory_space=pl.ANY)],
        out_specs=pl.BlockSpec(memory_space=pltpu.VMEM),
        scratch_shapes=[pltpu.SemaphoreType.DMA((8,))],
        name="sort_mats",
    )(kpoint_index.reshape(1), near, mats)


def rows_in_order(ref, holder):
    blocks = []
    for r in range(8):
        d = jnp.bitwise_xor(holder, r)
        at = 4 * jnp.bitwise_and(d, 1) + jnp.bitwise_and(d, 2) + jnp.right_shift(d, 2)
        blocks.append(ref[at])
    return jnp.concatenate(blocks, 0)


def main_kernel(w_ref, holder_ref, m_ref, u_ref, n_ref, z_ref, omega_ref):
    w = w_ref[0]
    a_r = m_ref[:, 0].reshape(512, 512)
    a_i = m_ref[:, 1].reshape(512, 512)
    u = rows_in_order(u_ref, holder_ref[0])
    n = rows_in_order(n_ref, holder_ref[1])
    half = jnp.right_shift(holder_ref[0], 2)
    ut = u.T
    p = dot_nt(ut, a_r)
    q = dot_nt(ut, a_i)
    qs = jnp.concatenate([p[:256] + q[256:], q[:256] - p[256:]], 0).astype(BF)
    p = dot(qs, n)
    mt_r = (p[:256, :256] - p[256:, 256:]).astype(BF)
    mt_i = (p[:256, 256:] + p[256:, :256]).astype(BF)
    mts = jnp.concatenate([mt_r, mt_i], 0)
    p = dot_nt(mts, n[:, :256])
    q = dot_nt(mts, n[:, 256:])
    vts = (w * jnp.concatenate([p[:256] + q[256:], q[:256] - p[256:]], 0)).astype(BF)
    p = dot_nt(mts, mts)
    h_r = w * (p[:256, :256] + p[256:, 256:])
    h_i = w * (p[256:, :256] - p[:256, 256:])
    mr, mi = mt_r.astype(F32), mt_i.astype(F32)
    row = lax.broadcasted_iota(jnp.int32, (256, 256), 0)
    col = lax.broadcasted_iota(jnp.int32, (256, 256), 1)
    eye = row == col
    zero = jnp.zeros_like(mr)
    only_r, only_i = jnp.where(eye, mr, zero), jnp.where(eye, mi, zero)
    row_r, row_i = only_r.sum(0, keepdims=True), only_i.sum(0, keepdims=True)
    col_r, col_i = only_r.sum(1, keepdims=True), only_i.sum(1, keepdims=True)
    tr, ti = mr.T, mi.T
    g_r = 2.0 * w * ((mr * row_r + mi * row_i) - (tr * col_r + ti * col_i))
    g_i = 2.0 * w * ((mi * row_r - mr * row_i) + (ti * col_r - tr * col_i))
    square = jnp.where(eye, zero, mr * mr + mi * mi)
    omega = jnp.sum(jnp.sum(square, 0, keepdims=True), 1, keepdims=True)
    omega_ref[...] = jnp.broadcast_to(omega * (w / (64 * 256)), omega_ref.shape)
    b_r, b_i = g_r.astype(BF), g_i.astype(BF)
    gt_r = -STEP_LENGTH * g_r - MIXING * h_r
    gt_i = STEP_LENGTH * g_i + MIXING * h_i
    gts = jnp.concatenate([gt_r, gt_i], 0).astype(BF)
    p = dot_nt(gts, u[:, :256])
    q = dot_nt(gts, u[:, 256:])
    zt_r = p[:256] - q[256:]
    zt_i = q[:256] + p[256:]
    p = dot(vts, a_r)
    q = dot(vts, a_i)
    zt_r = (zt_r + MIXING * (p[:256] - q[256:])).astype(BF)
    zt_i = (zt_i + MIXING * (q[:256] + p[256:])).astype(BF)
    z_r, z_i = zt_r.T, zt_i.T
    for h in range(2):
        for l in range(4):
            to = jnp.bitwise_xor(half, h)
            at = 64 * (4 * h + l)
            z_ref[l, to, :64, :256] = z_r[at : at + 64]
            z_ref[l, to, :64, 256:] = z_i[at : at + 64]
            at = 32 * (4 * h + l)
            z_ref[l, to, 64:, :256] = b_r[at : at + 32]
            z_ref[l, to, 64:, 256:] = b_i[at : at + 32]


def main_products(w, holders, mats, full, near):
    vmem = pl.BlockSpec(memory_space=pltpu.VMEM)
    smem = pl.BlockSpec(memory_space=pltpu.SMEM)
    return pl.pallas_call(
        main_kernel,
        out_shape=(
            jax.ShapeDtypeStruct((4, 2, 96, 512), BF),
            jax.ShapeDtypeStruct((8, 128), F32),
        ),
        in_specs=[smem, smem, vmem, vmem, vmem],
        out_specs=(vmem, vmem),
        compiler_params=pltpu.CompilerParams(vmem_limit_bytes=48 << 20),
        name="main_products",
    )(w.reshape(1), holders, mats, full, near)


def cdot(ar, ai, br, bi):
    p = dot(
        jnp.concatenate([ar, ai], 0).astype(BF), jnp.concatenate([br, bi], 1).astype(BF)
    )
    rows, cols = ar.shape[0], br.shape[1]
    return p[:rows, :cols] - p[rows:, cols:], p[:rows, cols:] + p[rows:, :cols]


def orth_kernel(x_ref, own_ref, out_ref):
    x = x_ref[...]
    p = dot(x.T, x)
    s_r = p[:256, :256] + p[256:, 256:]
    s_i = p[:256, 256:] - p[256:, :256]
    row = lax.broadcasted_iota(jnp.int32, (256, 256), 0)
    col = lax.broadcasted_iota(jnp.int32, (256, 256), 1)
    eye = (row == col).astype(F32)
    trace = jnp.sum(jnp.sum(s_r * eye, 0, keepdims=True), 1, keepdims=True)
    square = 256 / (2.0 * trace)
    scale = jnp.sqrt(square)
    d_r = 0.5 * (eye - square * s_r)
    d_i = -0.5 * (square * s_i)
    p_r, p_i = d_r, d_i
    for _ in range(2):
        q_r, q_i = cdot(d_r, d_i, d_r, d_i)
        c_r, c_i = cdot(q_r, q_i, d_r, d_i)
        d_r, d_i = 1.5 * q_r + c_r, 1.5 * q_i + c_i
        e_r, e_i = cdot(p_r, p_i, d_r, d_i)
        p_r, p_i = p_r + d_r + e_r, p_i + d_i + e_i
    own = own_ref[...]
    o_r, o_i = own[:, :256], own[:, 256:]
    e_r, e_i = cdot(o_r, o_i, p_r, p_i)
    out_ref[:, :256] = scale * (o_r + e_r)
    out_ref[:, 256:] = scale * (o_i + e_i)


def orthonormalized(full, own):
    vmem = pl.BlockSpec(memory_space=pltpu.VMEM)
    return pl.pallas_call(
        orth_kernel,
        out_shape=jax.ShapeDtypeStruct((64, 512), F32),
        in_specs=[vmem, vmem],
        out_specs=vmem,
        compiler_params=pltpu.CompilerParams(vmem_limit_bytes=48 << 20),
        name="orthonormalize",
    )(full, own)


def within_half(x):
    return lax.all_to_all(x, "col", 0, 0, tiled=True, axis_index_groups=HALVES)


def partner(x, axis, bit):
    length = lax.axis_size(axis)
    return lax.ppermute(x, axis, [(i, i ^ bit) for i in range(length)])


def per_device(correlations, gauge, neighbours, shifts):
    kpoint_index = lax.axis_index("ka")
    cindex = lax.axis_index("col")
    near, shift = neighbours[0], shifts[0]

    own = gauge[0].reshape(64, 512)
    mats = sorted_by_owner(kpoint_index, near, correlations[0])
    mats = lax.all_to_all(mats, "col", 0, 0, tiled=True)
    pair = jnp.stack([own, partner(own, "col", 4)])
    full = jnp.stack([pair, partner(pair, "col", 2)])
    full = jnp.stack([full, partner(full, "col", 1)]).reshape(8, 64, 512)
    near_full = lax.ppermute(full, ("ka", "col"), fetch_permutation())
    outer = jnp.logical_or(cindex == 0, cindex == 7)
    holders = jnp.stack([cindex, jnp.where(outer, 7 - cindex, cindex)])

    owners = owner_of(kpoint_index, *difference(near, kpoint_index))
    weights = shell_vector_weights(kpoint_index, near, shift)
    weight = jnp.sum(jnp.where(owners == cindex, weights, 0.0))

    z, spread = main_products(weight, holders, mats, full, near_full)

    z = within_half(z)
    for bit in (1, 2, 4, 16):
        spread = spread + partner(spread, "ka", bit)
    z = z.astype(F32).sum(0)
    arrived = jnp.concatenate([z[0, :64], z[1]], 0).astype(BF)
    arrived = partner(arrived, "col", 4).astype(F32)
    spread = spread + partner(spread, "ka", 32)
    groups = [
        [8 * (16 * y + 8 * h + x) + c for h in range(2) for c in range(8)]
        for y in range(4)
        for x in range(8)
    ]
    spread = lax.all_to_all(
        jnp.concatenate([spread, spread], 0),
        ("ka", "col"),
        0,
        0,
        tiled=True,
        axis_index_groups=groups,
    ).sum(0)
    x = pair.astype(F32) + jnp.stack([z[0, :64] + arrived[64:128], z[1, :64] + arrived[:64]])
    g = z[0, 64:] + arrived[128:]
    full_x = x.astype(BF).reshape(128, 512)
    for bit in (2, 1):
        full_x = jnp.concatenate([full_x, partner(full_x, "col", bit)], 0)
    own_x = x[0]
    u_next = orthonormalized(full_x, own_x)
    gradient = jnp.stack([g[:, :256], g[:, 256:]])[None]
    return (u_next.reshape(1, 64, 2, 256), gradient, spread[0])


def solution(mesh):
    return jax.shard_map(
        per_device,
        mesh=mesh,
        in_specs=(
            P("ka", None, None, "col", None),
            P("ka", "col", None, None),
            P("ka", None),
            P("ka", None, None),
        ),
        out_specs=(P("ka", "col", None, None), P("ka", None, "col", None), P()),
        check_vma=False,
    )
```

```python
import jax
import jax.numpy as jnp
from jax import lax
from jax.experimental import pallas as pl
from jax.experimental.pallas import tpu as pltpu
from jax.sharding import PartitionSpec as P


MIXING = 0.02
STEP_LENGTH = 0.2
SHELL_LIST = [
    (1, 0, 0),
    (-1, 0, 0),
    (0, 1, 0),
    (0, -1, 0),
    (0, 0, 1),
    (0, 0, -1),
    (1, 1, 1),
    (-1, -1, -1),
]
HALVES = [[0, 1, 2, 3], [4, 5, 6, 7]]
F32 = jnp.float32
BF = jnp.bfloat16


def dot(a, b):
    return lax.dot_general(a, b, (((1,), (0,)), ((), ())), preferred_element_type=F32)


def dot_nt(a, b):
    return lax.dot_general(a, b, (((1,), (1,)), ((), ())), preferred_element_type=F32)


def grid_positions(index):
    return jnp.stack([index // 16, index // 4 % 4, index % 4], -1)


def shell_vector_weights(kpoint_index, neighbour_list, shifts):
    grid_sizes = jnp.array([4, 4, 4], F32)
    f = (grid_positions(neighbour_list) - grid_positions(kpoint_index)[..., None, :]).astype(
        F32
    ) / grid_sizes
    f = f + shifts.astype(F32)
    cx = -f[..., 0] + f[..., 1] + f[..., 2]
    cy = f[..., 0] - f[..., 1] + f[..., 2]
    cz = f[..., 0] + f[..., 1] - f[..., 2]
    return 3.0 / (len(SHELL_LIST) * (cx * cx + cy * cy + cz * cz))


def owner_of(k, dx, dy, dz):
    diagonal = jnp.logical_and(dx != 0, dy != 0)
    plus = dx + dy + dz == jnp.where(diagonal, 3, 1)
    crosses = plus == ((k // 4) % 2 == 1)
    minus = jnp.where(plus, 0, 1)
    return jnp.where(
        diagonal,
        jnp.where(crosses, 7, 6),
        jnp.where(
            dy != 0,
            jnp.where(crosses, 0, 1),
            jnp.where(dx != 0, 2 + minus, 4 + minus),
        ),
    )


def difference(near, k):
    return (
        (near // 16 - k // 16 + 4) % 4,
        (near // 4 % 4 - k // 4 % 4 + 4) % 4,
        (near % 4 - k % 4 + 4) % 4,
    )


def fetch_permutation():
    pairs = []
    for k in range(64):
        for d in SHELL_LIST:
            g = [(a + b) % 4 for a, b in zip((k // 16, k // 4 % 4, k % 4), d)]
            plus = sum(d) > 0
            crosses = d[1] != 0 and plus == (k // 4 % 2 == 1)
            if d[0] and d[1]:
                c = 7 if crosses else 6
            elif d[1]:
                c = 0 if crosses else 1
            else:
                c = (2 if d[0] else 4) + (0 if plus else 1)
            source = 7 - c if crosses else c
            pairs.append(((g[0] * 16 + g[1] * 4 + g[2]) * 8 + source, k * 8 + c))
    return pairs


EARLY = 16


def sort_kernel(k_ref, near_ref, m_ref, early_ref, late_ref, sems):
    k = k_ref[0]
    copies = []
    for b in range(8):
        slot = owner_of(k, *difference(near_ref[b], k))
        for part, (out_ref, rows) in enumerate(
            ((early_ref, pl.ds(0, EARLY)), (late_ref, pl.ds(EARLY, 64 - EARLY)))
        ):
            copy = pltpu.make_async_copy(
                m_ref.at[b, :, rows], out_ref.at[slot], sems.at[part, b]
            )
            copy.start()
            copies.append(copy)
    for copy in copies:
        copy.wait()


def sorted_by_owner(kpoint_index, near, mats):
    smem = pl.BlockSpec(memory_space=pltpu.SMEM)
    vmem = pl.BlockSpec(memory_space=pltpu.VMEM)
    return pl.pallas_call(
        sort_kernel,
        out_shape=(
            jax.ShapeDtypeStruct((8, 2, EARLY, 512), BF),
            jax.ShapeDtypeStruct((8, 2, 64 - EARLY, 512), BF),
        ),
        in_specs=[smem, smem, pl.BlockSpec(memory_space=pl.ANY)],
        out_specs=(vmem, vmem),
        scratch_shapes=[pltpu.SemaphoreType.DMA((2, 8))],
        name="sort_mats",
    )(kpoint_index.reshape(1), near, mats)


def rows_in_order(ref, holder):
    blocks = []
    for r in range(8):
        d = jnp.bitwise_xor(holder, r)
        at = 4 * jnp.bitwise_and(d, 1) + jnp.bitwise_and(d, 2) + jnp.right_shift(d, 2)
        blocks.append(ref[at])
    return jnp.concatenate(blocks, 0)


def main_kernel(w_ref, holder_ref, early_ref, late_ref, u_ref, n_ref, z_ref):
    w = w_ref[0]
    a_r, a_i = (
        jnp.concatenate([ref[r, p] for r in range(8) for ref in (early_ref, late_ref)], 0)
        for p in range(2)
    )
    u = rows_in_order(u_ref, holder_ref[0])
    n = rows_in_order(n_ref, holder_ref[1])
    half = jnp.right_shift(holder_ref[0], 2)
    ut = u.T
    p = dot_nt(ut, a_r)
    q = dot_nt(ut, a_i)
    qs = jnp.concatenate([p[:256] + q[256:], q[:256] - p[256:]], 0).astype(BF)
    p = dot(qs, n)
    mt_r = (p[:256, :256] - p[256:, 256:]).astype(BF)
    mt_i = (p[:256, 256:] + p[256:, :256]).astype(BF)
    mts = jnp.concatenate([mt_r, mt_i], 0)
    p = dot_nt(mts, n[:, :256])
    q = dot_nt(mts, n[:, 256:])
    vts = (w * jnp.concatenate([p[:256] + q[256:], q[:256] - p[256:]], 0)).astype(BF)
    p = dot_nt(mts, mts)
    h_r = w * (p[:256, :256] + p[256:, 256:])
    h_i = w * (p[256:, :256] - p[:256, 256:])
    mr, mi = mt_r.astype(F32), mt_i.astype(F32)
    row = lax.broadcasted_iota(jnp.int32, (256, 256), 0)
    col = lax.broadcasted_iota(jnp.int32, (256, 256), 1)
    eye = row == col
    zero = jnp.zeros_like(mr)
    only_r, only_i = jnp.where(eye, mr, zero), jnp.where(eye, mi, zero)
    row_r, row_i = only_r.sum(0, keepdims=True), only_i.sum(0, keepdims=True)
    col_r, col_i = only_r.sum(1, keepdims=True), only_i.sum(1, keepdims=True)
    tr, ti = mr.T, mi.T
    g_r = 2.0 * w * ((mr * row_r + mi * row_i) - (tr * col_r + ti * col_i))
    g_i = 2.0 * w * ((mi * row_r - mr * row_i) + (ti * col_r - tr * col_i))
    square = jnp.where(eye, zero, mr * mr + mi * mi)
    omega = jnp.sum(jnp.sum(square, 0, keepdims=True), 1, keepdims=True)
    omega = omega * (w / (64 * 256))
    b_r = jnp.where(eye & (row % 32 == 0), omega, g_r).astype(BF)
    b_i = g_i.astype(BF)
    gt_r = -STEP_LENGTH * g_r - MIXING * h_r
    gt_i = STEP_LENGTH * g_i + MIXING * h_i
    gts = jnp.concatenate([gt_r, gt_i], 0).astype(BF)
    p = dot_nt(gts, u[:, :256])
    q = dot_nt(gts, u[:, 256:])
    zt_r = p[:256] - q[256:]
    zt_i = q[:256] + p[256:]
    p = dot(vts, a_r)
    q = dot(vts, a_i)
    zt_r = (zt_r + MIXING * (p[:256] - q[256:])).astype(BF)
    zt_i = (zt_i + MIXING * (q[:256] + p[256:])).astype(BF)
    z_r, z_i = zt_r.T, zt_i.T
    for h in range(2):
        for l in range(4):
            to = jnp.bitwise_xor(half, h)
            at = 64 * (4 * h + l)
            z_ref[l, to, :64, :256] = z_r[at : at + 64]
            z_ref[l, to, :64, 256:] = z_i[at : at + 64]
            at = 32 * (4 * h + l)
            z_ref[l, to, 64:, :256] = b_r[at : at + 32]
            z_ref[l, to, 64:, 256:] = b_i[at : at + 32]


def main_products(w, holders, early, late, full, near):
    vmem = pl.BlockSpec(memory_space=pltpu.VMEM)
    smem = pl.BlockSpec(memory_space=pltpu.SMEM)
    return pl.pallas_call(
        main_kernel,
        out_shape=jax.ShapeDtypeStruct((4, 2, 96, 512), BF),
        in_specs=[smem, smem, vmem, vmem, vmem, vmem],
        out_specs=vmem,
        compiler_params=pltpu.CompilerParams(vmem_limit_bytes=48 << 20),
        name="main_products",
    )(w.reshape(1), holders, early, late, full, near)


def cdot(ar, ai, br, bi):
    p = dot(
        jnp.concatenate([ar, ai], 0).astype(BF), jnp.concatenate([br, bi], 1).astype(BF)
    )
    rows, cols = ar.shape[0], br.shape[1]
    return p[:rows, :cols] - p[rows:, cols:], p[:rows, cols:] + p[rows:, :cols]


def orth_kernel(x_ref, own_ref, out_ref):
    x = x_ref[...]
    p = dot(x.T, x)
    s_r = p[:256, :256] + p[256:, 256:]
    s_i = p[:256, 256:] - p[256:, :256]
    row = lax.broadcasted_iota(jnp.int32, (256, 256), 0)
    col = lax.broadcasted_iota(jnp.int32, (256, 256), 1)
    eye = (row == col).astype(F32)
    trace = jnp.sum(jnp.sum(s_r * eye, 0, keepdims=True), 1, keepdims=True)
    square = 256 / (2.0 * trace)
    scale = jnp.sqrt(square)
    d_r = 0.5 * (eye - square * s_r)
    d_i = -0.5 * (square * s_i)
    p_r, p_i = d_r, d_i
    for _ in range(2):
        q_r, q_i = cdot(d_r, d_i, d_r, d_i)
        c_r, c_i = cdot(q_r, q_i, d_r, d_i)
        d_r, d_i = 1.5 * q_r + c_r, 1.5 * q_i + c_i
        e_r, e_i = cdot(p_r, p_i, d_r, d_i)
        p_r, p_i = p_r + d_r + e_r, p_i + d_i + e_i
    own = own_ref[...]
    o_r, o_i = own[:, :256], own[:, 256:]
    e_r, e_i = cdot(o_r, o_i, p_r, p_i)
    out_ref[:, 0] = scale * (o_r + e_r)
    out_ref[:, 1] = scale * (o_i + e_i)


def orthonormalized(full, own):
    vmem = pl.BlockSpec(memory_space=pltpu.VMEM)
    return pl.pallas_call(
        orth_kernel,
        out_shape=jax.ShapeDtypeStruct((64, 2, 256), F32),
        in_specs=[vmem, vmem],
        out_specs=vmem,
        compiler_params=pltpu.CompilerParams(vmem_limit_bytes=48 << 20),
        name="orthonormalize",
    )(full, own)


def within_half(x):
    return lax.all_to_all(x, "col", 0, 0, tiled=True, axis_index_groups=HALVES)


def partner(x, axis, bit):
    length = lax.axis_size(axis)
    return lax.ppermute(x, axis, [(i, i ^ bit) for i in range(length)])


def half_ring_permutation():
    pairs = []
    for k in range(64):
        for c in range(8):
            pairs.append((8 * k + c, 8 * (k ^ 8) + (c ^ 4)))
    return pairs


def per_device(correlations, gauge, neighbours, shifts):
    kpoint_index = lax.axis_index("ka")
    cindex = lax.axis_index("col")
    near, shift = neighbours[0], shifts[0]

    own = gauge[0].reshape(64, 512)
    early, late = sorted_by_owner(kpoint_index, near, correlations[0])
    early = lax.all_to_all(early, "col", 0, 0, tiled=True)
    late = lax.all_to_all(late, "col", 0, 0, tiled=True)
    pair = jnp.stack([own, partner(own, "col", 4)])
    full = jnp.stack([pair, partner(pair, "col", 2)])
    full = jnp.stack([full, partner(full, "col", 1)]).reshape(8, 64, 512)
    near_full = lax.ppermute(full, ("ka", "col"), fetch_permutation())
    outer = jnp.logical_or(cindex == 0, cindex == 7)
    holders = jnp.stack([cindex, jnp.where(outer, 7 - cindex, cindex)])

    owners = owner_of(kpoint_index, *difference(near, kpoint_index))
    weights = shell_vector_weights(kpoint_index, near, shift)
    weight = jnp.sum(jnp.where(owners == cindex, weights, 0.0))

    z = main_products(weight, holders, early, late, full, near_full)

    z = within_half(z).astype(F32).sum(0)
    arrived = jnp.concatenate([z[0, :64], z[1]], 0).astype(BF)
    arrived = partner(arrived, "col", 4).astype(F32)
    x = pair.astype(F32) + z[:, :64] + jnp.stack([arrived[64:128], arrived[:64]])
    full_x = x.astype(BF).reshape(128, 512)
    for bit in (2, 1):
        full_x = jnp.concatenate([full_x, partner(full_x, "col", bit)], 0)
    carries = jnp.arange(256)[None] == 32 * cindex
    groups = [[16 * y + 8 * z_hi + x for y in range(4) for x in range(8)] for z_hi in range(2)]
    spread = jnp.broadcast_to(jnp.where(carries, z[0, 64:65, :256], 0.0), (32, 256))
    spread = lax.all_to_all(spread, "ka", 0, 0, tiled=True, axis_index_groups=groups)
    spread = jnp.broadcast_to(spread.sum(0, keepdims=True), (8, 256))
    spread = spread + partner(spread, "col", 4)
    spread = spread + lax.ppermute(spread, ("ka", "col"), half_ring_permutation())
    u_next = orthonormalized(full_x, x[0])
    g = z[0, 64:] + arrived[128:]
    first = jnp.logical_and(carries, jnp.arange(32)[:, None] == 0)
    gradient = jnp.stack([jnp.where(first, 0.0, g[:, :256]), g[:, 256:]])[None]
    return (u_next[None], gradient, jnp.sum(spread[0]))


def solution(mesh):
    return jax.shard_map(
        per_device,
        mesh=mesh,
        in_specs=(
            P("ka", None, None, "col", None),
            P("ka", "col", None, None),
            P("ka", None),
            P("ka", None, None),
        ),
        out_specs=(P("ka", "col", None, None), P("ka", None, "col", None), P()),
        check_vma=False,
    )
```

```python
import functools

import jax
import jax.numpy as jnp
from jax import lax
from jax.experimental import pallas as pl
from jax.experimental.pallas import tpu as pltpu
from jax.sharding import PartitionSpec as P


MIXING = 0.02
STEP_LENGTH = 0.2
SHELL_LIST = [
    (1, 0, 0),
    (-1, 0, 0),
    (0, 1, 0),
    (0, -1, 0),
    (0, 0, 1),
    (0, 0, -1),
    (1, 1, 1),
    (-1, -1, -1),
]
HALVES = [[0, 1, 2, 3], [4, 5, 6, 7]]
F32 = jnp.float32
BF = jnp.bfloat16


def dot(a, b):
    return lax.dot_general(a, b, (((1,), (0,)), ((), ())), preferred_element_type=F32)


def dot_nt(a, b):
    return lax.dot_general(a, b, (((1,), (1,)), ((), ())), preferred_element_type=F32)


def grid_positions(index):
    return jnp.stack([index // 16, index // 4 % 4, index % 4], -1)


def shell_vector_weights(kpoint_index, neighbour_list, shifts):
    grid_sizes = jnp.array([4, 4, 4], F32)
    f = (grid_positions(neighbour_list) - grid_positions(kpoint_index)[..., None, :]).astype(
        F32
    ) / grid_sizes
    f = f + shifts.astype(F32)
    cx = -f[..., 0] + f[..., 1] + f[..., 2]
    cy = f[..., 0] - f[..., 1] + f[..., 2]
    cz = f[..., 0] + f[..., 1] - f[..., 2]
    return 3.0 / (len(SHELL_LIST) * (cx * cx + cy * cy + cz * cz))


def owner_of(k, dx, dy, dz):
    diagonal = jnp.logical_and(dx != 0, dy != 0)
    plus = dx + dy + dz == jnp.where(diagonal, 3, 1)
    crosses = plus == ((k // 4) % 2 == 1)
    minus = jnp.where(plus, 0, 1)
    return jnp.where(
        diagonal,
        jnp.where(crosses, 7, 6),
        jnp.where(
            dy != 0,
            jnp.where(crosses, 0, 1),
            jnp.where(dx != 0, 2 + minus, 4 + minus),
        ),
    )


def difference(near, k):
    return (
        (near // 16 - k // 16 + 4) % 4,
        (near // 4 % 4 - k // 4 % 4 + 4) % 4,
        (near % 4 - k % 4 + 4) % 4,
    )


def fetch_permutation():
    pairs = []
    for k in range(64):
        for d in SHELL_LIST:
            g = [(a + b) % 4 for a, b in zip((k // 16, k // 4 % 4, k % 4), d)]
            plus = sum(d) > 0
            crosses = d[1] != 0 and plus == (k // 4 % 2 == 1)
            if d[0] and d[1]:
                c = 7 if crosses else 6
            elif d[1]:
                c = 0 if crosses else 1
            else:
                c = (2 if d[0] else 4) + (0 if plus else 1)
            source = 7 - c if crosses else c
            pairs.append(((g[0] * 16 + g[1] * 4 + g[2]) * 8 + source, k * 8 + c))
    return pairs


EARLY = 32


def sort_kernel(k_ref, near_ref, m_ref, out_ref, sems, *, start):
    k = k_ref[0]
    copies = []
    for b in range(8):
        slot = owner_of(k, *difference(near_ref[b], k))
        rows = pl.ds(start, out_ref.shape[2])
        copy = pltpu.make_async_copy(m_ref.at[b, :, rows], out_ref.at[slot], sems.at[b])
        copy.start()
        copies.append(copy)
    for copy in copies:
        copy.wait()


def sorted_by_owner(kpoint_index, near, mats, start, rows):
    smem = pl.BlockSpec(memory_space=pltpu.SMEM)
    return pl.pallas_call(
        functools.partial(sort_kernel, start=start),
        out_shape=jax.ShapeDtypeStruct((8, 2, rows, 512), BF),
        in_specs=[smem, smem, pl.BlockSpec(memory_space=pl.ANY)],
        out_specs=pl.BlockSpec(memory_space=pltpu.VMEM),
        scratch_shapes=[pltpu.SemaphoreType.DMA((8,))],
        name="sort_mats",
    )(kpoint_index.reshape(1), near, mats)


def blocks_in_order(ref, holder):
    blocks = []
    for r in range(8):
        d = jnp.bitwise_xor(holder, r)
        at = 4 * jnp.bitwise_and(d, 1) + jnp.bitwise_and(d, 2) + jnp.right_shift(d, 2)
        blocks.append(ref[at])
    return blocks


def part(ref, p):
    return ref[:, p].reshape(8 * ref.shape[2], 512)


def conj_left(p, q):
    return jnp.concatenate([p[:256] + q[256:], q[:256] - p[256:]], 0)


def overlap(ut, mats_ref, near):
    qs = conj_left(dot_nt(ut, part(mats_ref, 0)), dot_nt(ut, part(mats_ref, 1))).astype(BF)
    p = dot(qs, near)
    return p[:256, :256] - p[256:, 256:], p[:256, 256:] + p[256:, :256]


def prep_kernel(holder_ref, early_ref, u_ref, n_ref, ut_ref, near_e_ref, near_l_ref, mt_ref):
    ut = jnp.concatenate(blocks_in_order(u_ref, holder_ref[0]), 0).T
    ut_ref[...] = ut
    blocks = blocks_in_order(n_ref, holder_ref[1])
    near_e = jnp.concatenate([block[:EARLY] for block in blocks], 0)
    near_e_ref[...] = near_e
    near_l_ref[...] = jnp.concatenate([block[EARLY:] for block in blocks], 0)
    mt_ref[0], mt_ref[1] = overlap(ut, early_ref, near_e)


def prepared(holders, early, full, near):
    vmem = pl.BlockSpec(memory_space=pltpu.VMEM)
    smem = pl.BlockSpec(memory_space=pltpu.SMEM)
    return pl.pallas_call(
        prep_kernel,
        out_shape=(
            jax.ShapeDtypeStruct((512, 512), BF),
            jax.ShapeDtypeStruct((8 * EARLY, 512), BF),
            jax.ShapeDtypeStruct((512 - 8 * EARLY, 512), BF),
            jax.ShapeDtypeStruct((2, 256, 256), F32),
        ),
        in_specs=[smem, vmem, vmem, vmem],
        out_specs=(vmem, vmem, vmem, vmem),
        compiler_params=pltpu.CompilerParams(vmem_limit_bytes=48 << 20),
        name="prep",
    )(holders, early, full, near)


def main_kernel(
    w_ref, holder_ref, early_ref, late_ref, ut_ref, near_e_ref, near_l_ref, mt_ref,
    z_ref, scratch_ref, sems,
):
    w = w_ref[0]
    half = jnp.right_shift(holder_ref[0], 2)
    ut = ut_ref[...]
    near_e, near_l = near_e_ref[...], near_l_ref[...]
    mt_r, mt_i = overlap(ut, late_ref, near_l)
    mt_r = (mt_ref[0] + mt_r).astype(BF)
    mt_i = (mt_ref[1] + mt_i).astype(BF)
    mts = jnp.concatenate([mt_r, mt_i], 0)
    vts_e, vts_l = (
        (w * conj_left(dot_nt(mts, near[:, :256]), dot_nt(mts, near[:, 256:]))).astype(BF)
        for near in (near_e, near_l)
    )
    p = dot_nt(mts, mts)
    h_r = w * (p[:256, :256] + p[256:, 256:])
    h_i = w * (p[256:, :256] - p[:256, 256:])
    mr, mi = mt_r.astype(F32), mt_i.astype(F32)
    row = lax.broadcasted_iota(jnp.int32, (256, 256), 0)
    col = lax.broadcasted_iota(jnp.int32, (256, 256), 1)
    eye = row == col
    zero = jnp.zeros_like(mr)
    only_r, only_i = jnp.where(eye, mr, zero), jnp.where(eye, mi, zero)
    row_r, row_i = only_r.sum(0, keepdims=True), only_i.sum(0, keepdims=True)
    col_r, col_i = only_r.sum(1, keepdims=True), only_i.sum(1, keepdims=True)
    tr, ti = mr.T, mi.T
    g_r = 2.0 * w * ((mr * row_r + mi * row_i) - (tr * col_r + ti * col_i))
    g_i = 2.0 * w * ((mi * row_r - mr * row_i) + (ti * col_r - tr * col_i))
    square = jnp.where(eye, zero, mr * mr + mi * mi)
    omega = jnp.sum(jnp.sum(square, 0, keepdims=True), 1, keepdims=True)
    omega = omega * (w / (64 * 256))
    b_r = jnp.where(eye & (row % 32 == 0), omega, g_r).astype(BF)
    b_i = g_i.astype(BF)
    copies = []

    def send(rows, lanes):
        piece = (slice(None), slice(None), rows, lanes)
        copy = pltpu.make_async_copy(
            scratch_ref.at[piece], z_ref.at[piece], sems.at[len(copies)]
        )
        copy.start()
        copies.append(copy)

    def store(value, rows, lanes):
        size = value.shape[0] // 8
        for h in range(2):
            to = jnp.bitwise_xor(half, h)
            for l in range(4):
                at = size * (4 * h + l)
                scratch_ref[l, to, rows, lanes] = value[at : at + size]

    low, high = pl.ds(0, 256), pl.ds(256, 256)
    store(b_r, pl.ds(64, 32), low)
    store(b_i, pl.ds(64, 32), high)
    send(pl.ds(64, 32), pl.ds(0, 512))
    gt_r = -STEP_LENGTH * g_r - MIXING * h_r
    gt_i = STEP_LENGTH * g_i + MIXING * h_i
    gts = jnp.concatenate([gt_r, gt_i], 0).astype(BF)
    p = dot(gts, ut[:256])
    q = dot(gts, ut[256:])
    y_p = dot(vts_e, part(early_ref, 0)) + dot(vts_l, part(late_ref, 0))
    y_q = dot(vts_e, part(early_ref, 1)) + dot(vts_l, part(late_ref, 1))
    z_r = (p[:256] - q[256:] + MIXING * (y_p[:256] - y_q[256:])).astype(BF)
    store(z_r.T, pl.ds(0, 64), low)
    send(pl.ds(0, 64), low)
    z_i = (q[:256] + p[256:] + MIXING * (y_q[:256] + y_p[256:])).astype(BF)
    store(z_i.T, pl.ds(0, 64), high)
    send(pl.ds(0, 64), high)
    for copy in copies:
        copy.wait()


def main_products(w, holders, early, late, prep):
    vmem = pl.BlockSpec(memory_space=pltpu.VMEM)
    smem = pl.BlockSpec(memory_space=pltpu.SMEM)
    return pl.pallas_call(
        main_kernel,
        out_shape=jax.ShapeDtypeStruct((4, 2, 96, 512), BF),
        in_specs=[smem, smem] + [vmem] * 6,
        out_specs=pl.BlockSpec(memory_space=pl.ANY),
        scratch_shapes=[pltpu.VMEM((4, 2, 96, 512), BF), pltpu.SemaphoreType.DMA((3,))],
        compiler_params=pltpu.CompilerParams(vmem_limit_bytes=48 << 20),
        name="main_products",
    )(w.reshape(1), holders, early, late, *prep)


def cdot(ar, ai, br, bi):
    p = dot(
        jnp.concatenate([ar, ai], 0).astype(BF), jnp.concatenate([br, bi], 1).astype(BF)
    )
    rows, cols = ar.shape[0], br.shape[1]
    return p[:rows, :cols] - p[rows:, cols:], p[:rows, cols:] + p[rows:, :cols]


def orth_kernel(x_ref, own_ref, out_ref):
    x = x_ref[...]
    p = dot(x.T, x)
    s_r = p[:256, :256] + p[256:, 256:]
    s_i = p[:256, 256:] - p[256:, :256]
    row = lax.broadcasted_iota(jnp.int32, (256, 256), 0)
    col = lax.broadcasted_iota(jnp.int32, (256, 256), 1)
    eye = (row == col).astype(F32)
    trace = jnp.sum(jnp.sum(s_r * eye, 0, keepdims=True), 1, keepdims=True)
    square = 256 / (2.0 * trace)
    scale = jnp.sqrt(square)
    d_r = 0.5 * (eye - square * s_r)
    d_i = -0.5 * (square * s_i)
    p_r, p_i = d_r, d_i
    for _ in range(2):
        q_r, q_i = cdot(d_r, d_i, d_r, d_i)
        c_r, c_i = cdot(q_r, q_i, d_r, d_i)
        d_r, d_i = 1.5 * q_r + c_r, 1.5 * q_i + c_i
        e_r, e_i = cdot(p_r, p_i, d_r, d_i)
        p_r, p_i = p_r + d_r + e_r, p_i + d_i + e_i
    own = own_ref[...]
    o_r, o_i = own[:, :256], own[:, 256:]
    e_r, e_i = cdot(o_r, o_i, p_r, p_i)
    out_ref[:, 0] = scale * (o_r + e_r)
    out_ref[:, 1] = scale * (o_i + e_i)


def orthonormalized(full, own):
    vmem = pl.BlockSpec(memory_space=pltpu.VMEM)
    return pl.pallas_call(
        orth_kernel,
        out_shape=jax.ShapeDtypeStruct((64, 2, 256), F32),
        in_specs=[vmem, vmem],
        out_specs=vmem,
        compiler_params=pltpu.CompilerParams(vmem_limit_bytes=48 << 20),
        name="orthonormalize",
    )(full, own)


def within_half(x):
    return lax.all_to_all(x, "col", 0, 0, tiled=True, axis_index_groups=HALVES)


def partner(x, axis, bit):
    length = lax.axis_size(axis)
    return lax.ppermute(x, axis, [(i, i ^ bit) for i in range(length)])


def half_ring_permutation():
    pairs = []
    for k in range(64):
        for c in range(8):
            pairs.append((8 * k + c, 8 * (k ^ 8) + (c ^ 4)))
    return pairs


def per_device(correlations, gauge, neighbours, shifts):
    kpoint_index = lax.axis_index("ka")
    cindex = lax.axis_index("col")
    near, shift = neighbours[0], shifts[0]

    own = gauge[0].reshape(64, 512)
    early = sorted_by_owner(kpoint_index, near, correlations[0], 0, EARLY)
    late = sorted_by_owner(kpoint_index, near, correlations[0], EARLY, 64 - EARLY)
    early = lax.all_to_all(early, "col", 0, 0, tiled=True)
    late = lax.all_to_all(late, "col", 0, 0, tiled=True)
    pair = jnp.stack([own, partner(own, "col", 4)])
    full = jnp.stack([pair, partner(pair, "col", 2)])
    full = jnp.stack([full, partner(full, "col", 1)]).reshape(8, 64, 512)
    near_full = lax.ppermute(full, ("ka", "col"), fetch_permutation())
    outer = jnp.logical_or(cindex == 0, cindex == 7)
    holders = jnp.stack([cindex, jnp.where(outer, 7 - cindex, cindex)])

    owners = owner_of(kpoint_index, *difference(near, kpoint_index))
    weights = shell_vector_weights(kpoint_index, near, shift)
    weight = jnp.sum(jnp.where(owners == cindex, weights, 0.0))

    prep = prepared(holders, early, full, near_full)
    z = main_products(weight, holders, early, late, prep)

    z = within_half(z).astype(F32).sum(0)
    arrived = jnp.concatenate([z[0, :64], z[1]], 0).astype(BF)
    arrived = partner(arrived, "col", 4).astype(F32)
    x = pair.astype(F32) + z[:, :64] + jnp.stack([arrived[64:128], arrived[:64]])
    full_x = x.astype(BF).reshape(128, 512)
    for bit in (2, 1):
        full_x = jnp.concatenate([full_x, partner(full_x, "col", bit)], 0)
    carries = jnp.arange(256)[None] == 32 * cindex
    groups = [[16 * y + 8 * z_hi + x for y in range(4) for x in range(8)] for z_hi in range(2)]
    spread = jnp.broadcast_to(jnp.where(carries, z[0, 64:65, :256], 0.0), (32, 256))
    spread = lax.all_to_all(spread, "ka", 0, 0, tiled=True, axis_index_groups=groups)
    spread = jnp.broadcast_to(spread.sum(0, keepdims=True), (8, 256))
    spread = spread + partner(spread, "col", 4)
    spread = spread + lax.ppermute(spread, ("ka", "col"), half_ring_permutation())
    u_next = orthonormalized(full_x, x[0])
    g = z[0, 64:] + arrived[128:]
    first = jnp.logical_and(carries, jnp.arange(32)[:, None] == 0)
    gradient = jnp.stack([jnp.where(first, 0.0, g[:, :256]), g[:, 256:]])[None]
    return (u_next[None], gradient, jnp.sum(spread[0]))


def solution(mesh):
    return jax.shard_map(
        per_device,
        mesh=mesh,
        in_specs=(
            P("ka", None, None, "col", None),
            P("ka", "col", None, None),
            P("ka", None),
            P("ka", None, None),
        ),
        out_specs=(P("ka", "col", None, None), P("ka", None, "col", None), P()),
        check_vma=False,
    )
```

```python
import functools

import jax
import jax.numpy as jnp
from jax import lax
from jax.experimental import pallas as pl
from jax.experimental.pallas import tpu as pltpu
from jax.sharding import PartitionSpec as P


MIXING = 0.02
STEP_LENGTH = 0.2
SHELL_LIST = [
    (1, 0, 0),
    (-1, 0, 0),
    (0, 1, 0),
    (0, -1, 0),
    (0, 0, 1),
    (0, 0, -1),
    (1, 1, 1),
    (-1, -1, -1),
]
HALVES = [[0, 1, 2, 3], [4, 5, 6, 7]]
F32 = jnp.float32
BF = jnp.bfloat16


def dot(a, b):
    return lax.dot_general(a, b, (((1,), (0,)), ((), ())), preferred_element_type=F32)


def dot_nt(a, b):
    return lax.dot_general(a, b, (((1,), (1,)), ((), ())), preferred_element_type=F32)


def grid_positions(index):
    return jnp.stack([index // 16, index // 4 % 4, index % 4], -1)


def shell_vector_weights(kpoint_index, neighbour_list, shifts):
    grid_sizes = jnp.array([4, 4, 4], F32)
    f = (grid_positions(neighbour_list) - grid_positions(kpoint_index)[..., None, :]).astype(
        F32
    ) / grid_sizes
    f = f + shifts.astype(F32)
    cx = -f[..., 0] + f[..., 1] + f[..., 2]
    cy = f[..., 0] - f[..., 1] + f[..., 2]
    cz = f[..., 0] + f[..., 1] - f[..., 2]
    return 3.0 / (len(SHELL_LIST) * (cx * cx + cy * cy + cz * cz))


def owner_of(k, dx, dy, dz):
    diagonal = jnp.logical_and(dx != 0, dy != 0)
    plus = dx + dy + dz == jnp.where(diagonal, 3, 1)
    crosses = plus == ((k // 4) % 2 == 1)
    minus = jnp.where(plus, 0, 1)
    return jnp.where(
        diagonal,
        jnp.where(crosses, 7, 6),
        jnp.where(
            dy != 0,
            jnp.where(crosses, 0, 1),
            jnp.where(dx != 0, 2 + minus, 4 + minus),
        ),
    )


def difference(near, k):
    return (
        (near // 16 - k // 16 + 4) % 4,
        (near // 4 % 4 - k // 4 % 4 + 4) % 4,
        (near % 4 - k % 4 + 4) % 4,
    )


def fetch_permutation():
    pairs = []
    for k in range(64):
        for d in SHELL_LIST:
            g = [(a + b) % 4 for a, b in zip((k // 16, k // 4 % 4, k % 4), d)]
            plus = sum(d) > 0
            crosses = d[1] != 0 and plus == (k // 4 % 2 == 1)
            if d[0] and d[1]:
                c = 7 if crosses else 6
            elif d[1]:
                c = 0 if crosses else 1
            else:
                c = (2 if d[0] else 4) + (0 if plus else 1)
            source = 7 - c if crosses else c
            pairs.append(((g[0] * 16 + g[1] * 4 + g[2]) * 8 + source, k * 8 + c))
    return pairs


EARLY = 32


def sort_kernel(k_ref, near_ref, m_ref, out_ref, sems, *, start):
    k = k_ref[0]
    copies = []
    for b in range(8):
        slot = owner_of(k, *difference(near_ref[b], k))
        rows = pl.ds(start, out_ref.shape[2])
        copy = pltpu.make_async_copy(m_ref.at[b, :, rows], out_ref.at[slot], sems.at[b])
        copy.start()
        copies.append(copy)
    for copy in copies:
        copy.wait()


def sorted_by_owner(kpoint_index, near, mats, start, rows):
    smem = pl.BlockSpec(memory_space=pltpu.SMEM)
    return pl.pallas_call(
        functools.partial(sort_kernel, start=start),
        out_shape=jax.ShapeDtypeStruct((8, 2, rows, 512), BF),
        in_specs=[smem, smem, pl.BlockSpec(memory_space=pl.ANY)],
        out_specs=pl.BlockSpec(memory_space=pltpu.VMEM),
        scratch_shapes=[pltpu.SemaphoreType.DMA((8,))],
        name="sort_mats",
    )(kpoint_index.reshape(1), near, mats)


def blocks_in_order(ref, holder):
    blocks = []
    for r in range(8):
        d = jnp.bitwise_xor(holder, r)
        at = 4 * jnp.bitwise_and(d, 1) + jnp.bitwise_and(d, 2) + jnp.right_shift(d, 2)
        blocks.append(ref[at])
    return blocks


def part(ref, p):
    return ref[:, p].reshape(8 * ref.shape[2], 512)


def conj_left(p, q):
    return jnp.concatenate([p[:256] + q[256:], q[:256] - p[256:]], 0)


def overlap(ut, mats_ref, near):
    qs = conj_left(dot_nt(ut, part(mats_ref, 0)), dot_nt(ut, part(mats_ref, 1))).astype(BF)
    p = dot(qs, near)
    return p[:256, :256] - p[256:, 256:], p[:256, 256:] + p[256:, :256]


def prep_kernel(holder_ref, early_ref, u_ref, n_ref, ut_ref, near_e_ref, near_l_ref, mt_ref):
    ut = jnp.concatenate(blocks_in_order(u_ref, holder_ref[0]), 0).T
    ut_ref[...] = ut
    blocks = blocks_in_order(n_ref, holder_ref[1])
    near_e = jnp.concatenate([block[:EARLY] for block in blocks], 0)
    near_e_ref[...] = near_e
    near_l_ref[...] = jnp.concatenate([block[EARLY:] for block in blocks], 0)
    mt_ref[0], mt_ref[1] = overlap(ut, early_ref, near_e)


def prepared(holders, early, full, near):
    vmem = pl.BlockSpec(memory_space=pltpu.VMEM)
    smem = pl.BlockSpec(memory_space=pltpu.SMEM)
    return pl.pallas_call(
        prep_kernel,
        out_shape=(
            jax.ShapeDtypeStruct((512, 512), BF),
            jax.ShapeDtypeStruct((8 * EARLY, 512), BF),
            jax.ShapeDtypeStruct((512 - 8 * EARLY, 512), BF),
            jax.ShapeDtypeStruct((2, 256, 256), F32),
        ),
        in_specs=[smem, vmem, vmem, vmem],
        out_specs=(vmem, vmem, vmem, vmem),
        compiler_params=pltpu.CompilerParams(vmem_limit_bytes=48 << 20),
        name="prep",
    )(holders, early, full, near)


def main_kernel(
    w_ref, holder_ref, early_ref, late_ref, ut_ref, near_e_ref, near_l_ref, mt_ref,
    z_ref, scratch_ref, sems,
):
    w = w_ref[0]
    half = jnp.right_shift(holder_ref[0], 2)
    ut = ut_ref[...]
    near_e, near_l = near_e_ref[...], near_l_ref[...]
    mt_r, mt_i = overlap(ut, late_ref, near_l)
    mt_r = (mt_ref[0] + mt_r).astype(BF)
    mt_i = (mt_ref[1] + mt_i).astype(BF)
    mts = jnp.concatenate([mt_r, mt_i], 0)
    vts_e, vts_l = (
        (w * conj_left(dot_nt(mts, near[:, :256]), dot_nt(mts, near[:, 256:]))).astype(BF)
        for near in (near_e, near_l)
    )
    p = dot_nt(mts, mts)
    h_r = w * (p[:256, :256] + p[256:, 256:])
    h_i = w * (p[256:, :256] - p[:256, 256:])
    mr, mi = mt_r.astype(F32), mt_i.astype(F32)
    row = lax.broadcasted_iota(jnp.int32, (256, 256), 0)
    col = lax.broadcasted_iota(jnp.int32, (256, 256), 1)
    eye = row == col
    zero = jnp.zeros_like(mr)
    only_r, only_i = jnp.where(eye, mr, zero), jnp.where(eye, mi, zero)
    row_r, row_i = only_r.sum(0, keepdims=True), only_i.sum(0, keepdims=True)
    col_r, col_i = only_r.sum(1, keepdims=True), only_i.sum(1, keepdims=True)
    tr, ti = mr.T, mi.T
    g_r = 2.0 * w * ((mr * row_r + mi * row_i) - (tr * col_r + ti * col_i))
    g_i = 2.0 * w * ((mi * row_r - mr * row_i) + (ti * col_r - tr * col_i))
    square = jnp.where(eye, zero, mr * mr + mi * mi)
    omega = jnp.sum(jnp.sum(square, 0, keepdims=True), 1, keepdims=True)
    omega = omega * (w / (64 * 256))
    b_r = jnp.where(eye & (row % 32 == 0), omega, g_r).astype(BF)
    b_i = g_i.astype(BF)
    copies = []

    def send(rows, lanes):
        piece = (slice(None), slice(None), rows, lanes)
        copy = pltpu.make_async_copy(
            scratch_ref.at[piece], z_ref.at[piece], sems.at[len(copies)]
        )
        copy.start()
        copies.append(copy)

    def store(value, rows, lanes):
        size = value.shape[0] // 8
        for h in range(2):
            to = jnp.bitwise_xor(half, h)
            for l in range(4):
                at = size * (4 * h + l)
                scratch_ref[l, to, rows, lanes] = value[at : at + size]

    low, high = pl.ds(0, 256), pl.ds(256, 256)
    store(b_r, pl.ds(64, 32), low)
    store(b_i, pl.ds(64, 32), high)
    send(pl.ds(64, 32), pl.ds(0, 512))
    gt_r = -STEP_LENGTH * g_r - MIXING * h_r
    gt_i = STEP_LENGTH * g_i + MIXING * h_i
    gts = jnp.concatenate([gt_r, gt_i], 0).astype(BF)
    p = dot(gts, ut[:256])
    q = dot(gts, ut[256:])
    y_p = dot(vts_e, part(early_ref, 0)) + dot(vts_l, part(late_ref, 0))
    y_q = dot(vts_e, part(early_ref, 1)) + dot(vts_l, part(late_ref, 1))
    z_r = (p[:256] - q[256:] + MIXING * (y_p[:256] - y_q[256:])).astype(BF)
    store(z_r.T, pl.ds(0, 64), low)
    send(pl.ds(0, 64), low)
    z_i = (q[:256] + p[256:] + MIXING * (y_q[:256] + y_p[256:])).astype(BF)
    store(z_i.T, pl.ds(0, 64), high)
    send(pl.ds(0, 64), high)
    for copy in copies:
        copy.wait()


def main_products(w, holders, early, late, prep):
    vmem = pl.BlockSpec(memory_space=pltpu.VMEM)
    smem = pl.BlockSpec(memory_space=pltpu.SMEM)
    return pl.pallas_call(
        main_kernel,
        out_shape=jax.ShapeDtypeStruct((4, 2, 96, 512), BF),
        in_specs=[smem, smem] + [vmem] * 6,
        out_specs=pl.BlockSpec(memory_space=pl.ANY),
        scratch_shapes=[pltpu.VMEM((4, 2, 96, 512), BF), pltpu.SemaphoreType.DMA((3,))],
        compiler_params=pltpu.CompilerParams(vmem_limit_bytes=48 << 20),
        name="main_products",
    )(w.reshape(1), holders, early, late, *prep)


def cdot(ar, ai, br, bi):
    p = dot(
        jnp.concatenate([ar, ai], 0).astype(BF), jnp.concatenate([br, bi], 1).astype(BF)
    )
    rows, cols = ar.shape[0], br.shape[1]
    return p[:rows, :cols] - p[rows:, cols:], p[:rows, cols:] + p[rows:, :cols]


def orth_kernel(x_ref, own_ref, out_ref):
    x = x_ref[...]
    p = dot(x.T, x)
    s_r = p[:256, :256] + p[256:, 256:]
    s_i = p[:256, 256:] - p[256:, :256]
    row = lax.broadcasted_iota(jnp.int32, (256, 256), 0)
    col = lax.broadcasted_iota(jnp.int32, (256, 256), 1)
    eye = (row == col).astype(F32)
    trace = jnp.sum(jnp.sum(s_r * eye, 0, keepdims=True), 1, keepdims=True)
    square = 256 / (2.0 * trace)
    scale = jnp.sqrt(square)
    d_r = 0.5 * (eye - square * s_r)
    d_i = -0.5 * (square * s_i)
    own = own_ref[...]
    y_r, y_i = own[:, :256], own[:, 256:]
    for turn in range(3):
        if turn:
            q_r, q_i = cdot(d_r, d_i, d_r, d_i)
            c_r, c_i = cdot(q_r, q_i, d_r, d_i)
            d_r, d_i = 1.5 * q_r + c_r, 1.5 * q_i + c_i
        e_r, e_i = cdot(y_r, y_i, d_r, d_i)
        y_r, y_i = y_r + e_r, y_i + e_i
    out_ref[:, 0] = scale * y_r
    out_ref[:, 1] = scale * y_i


def orthonormalized(full, own):
    vmem = pl.BlockSpec(memory_space=pltpu.VMEM)
    return pl.pallas_call(
        orth_kernel,
        out_shape=jax.ShapeDtypeStruct((64, 2, 256), F32),
        in_specs=[vmem, vmem],
        out_specs=vmem,
        compiler_params=pltpu.CompilerParams(vmem_limit_bytes=48 << 20),
        name="orthonormalize",
    )(full, own)


def within_half(x):
    return lax.all_to_all(x, "col", 0, 0, tiled=True, axis_index_groups=HALVES)


def partner(x, axis, bit):
    length = lax.axis_size(axis)
    return lax.ppermute(x, axis, [(i, i ^ bit) for i in range(length)])


def half_ring_permutation():
    pairs = []
    for k in range(64):
        for c in range(8):
            pairs.append((8 * k + c, 8 * (k ^ 8) + (c ^ 4)))
    return pairs


def per_device(correlations, gauge, neighbours, shifts):
    kpoint_index = lax.axis_index("ka")
    cindex = lax.axis_index("col")
    near, shift = neighbours[0], shifts[0]

    own = lax.optimization_barrier(gauge[0].reshape(64, 512))
    early = sorted_by_owner(kpoint_index, near, correlations[0], 0, EARLY)
    late = sorted_by_owner(kpoint_index, near, correlations[0], EARLY, 64 - EARLY)
    early = lax.all_to_all(early, "col", 0, 0, tiled=True)
    late = lax.all_to_all(late, "col", 0, 0, tiled=True)
    pair = jnp.stack([own, partner(own, "col", 4)])
    full = jnp.stack([pair, partner(pair, "col", 2)])
    full = jnp.stack([full, partner(full, "col", 1)]).reshape(8, 64, 512)
    near_full = lax.ppermute(full, ("ka", "col"), fetch_permutation())
    outer = jnp.logical_or(cindex == 0, cindex == 7)
    holders = jnp.stack([cindex, jnp.where(outer, 7 - cindex, cindex)])

    owners = owner_of(kpoint_index, *difference(near, kpoint_index))
    weights = shell_vector_weights(kpoint_index, near, shift)
    weight = jnp.sum(jnp.where(owners == cindex, weights, 0.0))

    prep = prepared(holders, early, full, near_full)
    z = main_products(weight, holders, early, late, prep)

    z = within_half(z).astype(F32).sum(0)
    arrived = jnp.concatenate([z[0, :64], z[1]], 0).astype(BF)
    arrived = partner(arrived, "col", 4).astype(F32)
    x = pair.astype(F32) + z[:, :64] + jnp.stack([arrived[64:128], arrived[:64]])
    full_x = x.astype(BF).reshape(128, 512)
    for bit in (2, 1):
        full_x = jnp.concatenate([full_x, partner(full_x, "col", bit)], 0)
    carries = jnp.arange(256)[None] == 32 * cindex
    groups = [[16 * y + 8 * z_hi + x for y in range(4) for x in range(8)] for z_hi in range(2)]
    spread = jnp.broadcast_to(jnp.where(carries, z[0, 64:65, :256], 0.0), (32, 256))
    spread = lax.all_to_all(spread, "ka", 0, 0, tiled=True, axis_index_groups=groups)
    spread = jnp.broadcast_to(spread.sum(0, keepdims=True), (8, 256))
    spread = spread + partner(spread, "col", 4)
    spread = spread + lax.ppermute(spread, ("ka", "col"), half_ring_permutation())
    u_next = orthonormalized(full_x, x[0])
    g = z[0, 64:] + arrived[128:]
    first = jnp.logical_and(carries, jnp.arange(32)[:, None] == 0)
    gradient = jnp.stack([jnp.where(first, 0.0, g[:, :256]), g[:, 256:]])[None]
    return (u_next[None], gradient, jnp.sum(spread[0]))


def solution(mesh):
    return jax.shard_map(
        per_device,
        mesh=mesh,
        in_specs=(
            P("ka", None, None, "col", None),
            P("ka", "col", None, None),
            P("ka", None),
            P("ka", None, None),
        ),
        out_specs=(P("ka", "col", None, None), P("ka", None, "col", None), P()),
        check_vma=False,
    )
```

```python
import functools

import jax
import jax.numpy as jnp
from jax import lax
from jax.experimental import pallas as pl
from jax.experimental.pallas import tpu as pltpu
from jax.sharding import PartitionSpec as P


MIXING = 0.02
STEP_LENGTH = 0.2
SHELL_LIST = [
    (1, 0, 0),
    (-1, 0, 0),
    (0, 1, 0),
    (0, -1, 0),
    (0, 0, 1),
    (0, 0, -1),
    (1, 1, 1),
    (-1, -1, -1),
]
HALVES = [[0, 1, 2, 3], [4, 5, 6, 7]]
F32 = jnp.float32
BF = jnp.bfloat16


def dot(a, b):
    return lax.dot_general(a, b, (((1,), (0,)), ((), ())), preferred_element_type=F32)


def dot_nt(a, b):
    return lax.dot_general(a, b, (((1,), (1,)), ((), ())), preferred_element_type=F32)


def grid_positions(index):
    return jnp.stack([index // 16, index // 4 % 4, index % 4], -1)


def shell_vector_weights(kpoint_index, neighbour_list, shifts):
    grid_sizes = jnp.array([4, 4, 4], F32)
    f = (grid_positions(neighbour_list) - grid_positions(kpoint_index)[..., None, :]).astype(
        F32
    ) / grid_sizes
    f = f + shifts.astype(F32)
    cx = -f[..., 0] + f[..., 1] + f[..., 2]
    cy = f[..., 0] - f[..., 1] + f[..., 2]
    cz = f[..., 0] + f[..., 1] - f[..., 2]
    return 3.0 / (len(SHELL_LIST) * (cx * cx + cy * cy + cz * cz))


def owner_of(k, dx, dy, dz):
    diagonal = jnp.logical_and(dx != 0, dy != 0)
    plus = dx + dy + dz == jnp.where(diagonal, 3, 1)
    crosses = plus == ((k // 4) % 2 == 1)
    minus = jnp.where(plus, 0, 1)
    return jnp.where(
        diagonal,
        jnp.where(crosses, 0, 1),
        jnp.where(
            dy != 0,
            jnp.where(crosses, 7, 6),
            jnp.where(dx != 0, 2 + minus, 4 + minus),
        ),
    )


def difference(near, k):
    return (
        (near // 16 - k // 16 + 4) % 4,
        (near // 4 % 4 - k // 4 % 4 + 4) % 4,
        (near % 4 - k % 4 + 4) % 4,
    )


def fetch_permutation():
    pairs = []
    for k in range(64):
        for d in SHELL_LIST:
            g = [(a + b) % 4 for a, b in zip((k // 16, k // 4 % 4, k % 4), d)]
            plus = sum(d) > 0
            crosses = d[1] != 0 and plus == (k // 4 % 2 == 1)
            if d[0] and d[1]:
                c = 0 if crosses else 1
            elif d[1]:
                c = 7 if crosses else 6
            else:
                c = (2 if d[0] else 4) + (0 if plus else 1)
            source = 7 - c if crosses else c
            pairs.append(((g[0] * 16 + g[1] * 4 + g[2]) * 8 + source, k * 8 + c))
    return pairs


EARLY = 32


def sort_kernel(k_ref, near_ref, m_ref, out_ref, block_ref, in_sems, out_sems, *, start):
    k = k_ref[0]
    arriving, leaving = [], []
    for b in range(8):
        rows = pl.ds(start, out_ref.shape[2])
        copy = pltpu.make_async_copy(m_ref.at[b, :, rows], block_ref.at[b], in_sems.at[b])
        copy.start()
        arriving.append(copy)
    for b in range(8):
        slot = owner_of(k, *difference(near_ref[b], k))
        arriving[b].wait()
        copy = pltpu.make_async_copy(block_ref.at[b], out_ref.at[slot], out_sems.at[b])
        copy.start()
        leaving.append(copy)
    for copy in leaving:
        copy.wait()


def sorted_by_owner(kpoint_index, near, mats, start, rows):
    smem = pl.BlockSpec(memory_space=pltpu.SMEM)
    return pl.pallas_call(
        functools.partial(sort_kernel, start=start),
        out_shape=jax.ShapeDtypeStruct((8, 2, rows, 512), BF),
        in_specs=[smem, smem, pl.BlockSpec(memory_space=pl.ANY)],
        out_specs=pl.BlockSpec(memory_space=pl.ANY),
        scratch_shapes=[
            pltpu.VMEM((8, 2, rows, 512), BF),
            pltpu.SemaphoreType.DMA((8,)),
            pltpu.SemaphoreType.DMA((8,)),
        ],
        name="sort_mats",
    )(kpoint_index.reshape(1), near, mats)


def blocks_in_order(ref, holder):
    blocks = []
    for r in range(8):
        d = jnp.bitwise_xor(holder, r)
        at = 4 * jnp.bitwise_and(d, 1) + jnp.bitwise_and(d, 2) + jnp.right_shift(d, 2)
        blocks.append(ref[at])
    return blocks


def part(ref, p):
    return ref[:, p].reshape(8 * ref.shape[2], 512)


def conj_left(p, q):
    return jnp.concatenate([p[:256] + q[256:], q[:256] - p[256:]], 0)


def overlap(ut, mats_ref, near):
    qs = conj_left(dot_nt(ut, part(mats_ref, 0)), dot_nt(ut, part(mats_ref, 1))).astype(BF)
    p = dot(qs, near)
    return p[:256, :256] - p[256:, 256:], p[:256, 256:] + p[256:, :256]


def prep_kernel(holder_ref, early_ref, u_ref, n_ref, ut_ref, near_e_ref, near_l_ref, mt_ref):
    ut = jnp.concatenate(blocks_in_order(u_ref, holder_ref[0]), 0).T
    ut_ref[...] = ut
    blocks = blocks_in_order(n_ref, holder_ref[1])
    near_e = jnp.concatenate([block[:EARLY] for block in blocks], 0)
    near_e_ref[...] = near_e
    near_l_ref[...] = jnp.concatenate([block[EARLY:] for block in blocks], 0)
    mt_ref[0], mt_ref[1] = overlap(ut, early_ref, near_e)


def prepared(holders, early, full, near):
    vmem = pl.BlockSpec(memory_space=pltpu.VMEM)
    smem = pl.BlockSpec(memory_space=pltpu.SMEM)
    return pl.pallas_call(
        prep_kernel,
        out_shape=(
            jax.ShapeDtypeStruct((512, 512), BF),
            jax.ShapeDtypeStruct((8 * EARLY, 512), BF),
            jax.ShapeDtypeStruct((512 - 8 * EARLY, 512), BF),
            jax.ShapeDtypeStruct((2, 256, 256), F32),
        ),
        in_specs=[smem, vmem, vmem, vmem],
        out_specs=(vmem, vmem, vmem, vmem),
        compiler_params=pltpu.CompilerParams(vmem_limit_bytes=48 << 20),
        name="prep",
    )(holders, early, full, near)


def main_kernel(
    w_ref, holder_ref, early_ref, late_ref, ut_ref, near_e_ref, near_l_ref, mt_ref,
    z_ref, scratch_ref, sems,
):
    w = w_ref[0]
    half = jnp.right_shift(holder_ref[0], 2)
    ut = ut_ref[...]
    near_e, near_l = near_e_ref[...], near_l_ref[...]
    mt_r, mt_i = overlap(ut, late_ref, near_l)
    mt_r = (mt_ref[0] + mt_r).astype(BF)
    mt_i = (mt_ref[1] + mt_i).astype(BF)
    mts = jnp.concatenate([mt_r, mt_i], 0)
    vts_e, vts_l = (
        (w * conj_left(dot_nt(mts, near[:, :256]), dot_nt(mts, near[:, 256:]))).astype(BF)
        for near in (near_e, near_l)
    )
    p = dot_nt(mts, mts)
    h_r = w * (p[:256, :256] + p[256:, 256:])
    h_i = w * (p[256:, :256] - p[:256, 256:])
    mr, mi = mt_r.astype(F32), mt_i.astype(F32)
    row = lax.broadcasted_iota(jnp.int32, (256, 256), 0)
    col = lax.broadcasted_iota(jnp.int32, (256, 256), 1)
    eye = row == col
    zero = jnp.zeros_like(mr)
    only_r, only_i = jnp.where(eye, mr, zero), jnp.where(eye, mi, zero)
    row_r, row_i = only_r.sum(0, keepdims=True), only_i.sum(0, keepdims=True)
    col_r, col_i = only_r.sum(1, keepdims=True), only_i.sum(1, keepdims=True)
    tr, ti = mr.T, mi.T
    g_r = 2.0 * w * ((mr * row_r + mi * row_i) - (tr * col_r + ti * col_i))
    g_i = 2.0 * w * ((mi * row_r - mr * row_i) + (ti * col_r - tr * col_i))
    square = jnp.where(eye, zero, mr * mr + mi * mi)
    omega = jnp.sum(jnp.sum(square, 0, keepdims=True), 1, keepdims=True)
    omega = omega * (w / (64 * 256))
    b_r = jnp.where(eye & (row % 32 == 0), omega, g_r).astype(BF)
    b_i = g_i.astype(BF)
    copies = []

    def send(rows, lanes):
        piece = (slice(None), slice(None), rows, lanes)
        copy = pltpu.make_async_copy(
            scratch_ref.at[piece], z_ref.at[piece], sems.at[len(copies)]
        )
        copy.start()
        copies.append(copy)

    def store(value, rows, lanes):
        size = value.shape[0] // 8
        for h in range(2):
            to = jnp.bitwise_xor(half, h)
            for l in range(4):
                at = size * (4 * h + l)
                scratch_ref[l, to, rows, lanes] = value[at : at + size]

    low, high = pl.ds(0, 256), pl.ds(256, 256)
    store(b_r, pl.ds(64, 32), low)
    store(b_i, pl.ds(64, 32), high)
    send(pl.ds(64, 32), pl.ds(0, 512))
    gt_r = -STEP_LENGTH * g_r - MIXING * h_r
    gt_i = STEP_LENGTH * g_i + MIXING * h_i
    gts = jnp.concatenate([gt_r, gt_i], 0).astype(BF)
    p = dot(gts, ut[:256])
    q = dot(gts, ut[256:])
    y_p = dot(vts_e, part(early_ref, 0)) + dot(vts_l, part(late_ref, 0))
    y_q = dot(vts_e, part(early_ref, 1)) + dot(vts_l, part(late_ref, 1))
    z_r = (p[:256] - q[256:] + MIXING * (y_p[:256] - y_q[256:])).astype(BF)
    store(z_r.T, pl.ds(0, 64), low)
    send(pl.ds(0, 64), low)
    z_i = (q[:256] + p[256:] + MIXING * (y_q[:256] + y_p[256:])).astype(BF)
    store(z_i.T, pl.ds(0, 64), high)
    send(pl.ds(0, 64), high)
    for copy in copies:
        copy.wait()


def main_products(w, holders, early, late, prep):
    vmem = pl.BlockSpec(memory_space=pltpu.VMEM)
    smem = pl.BlockSpec(memory_space=pltpu.SMEM)
    return pl.pallas_call(
        main_kernel,
        out_shape=jax.ShapeDtypeStruct((4, 2, 96, 512), BF),
        in_specs=[smem, smem] + [vmem] * 6,
        out_specs=pl.BlockSpec(memory_space=pl.ANY),
        scratch_shapes=[pltpu.VMEM((4, 2, 96, 512), BF), pltpu.SemaphoreType.DMA((3,))],
        compiler_params=pltpu.CompilerParams(vmem_limit_bytes=48 << 20),
        name="main_products",
    )(w.reshape(1), holders, early, late, *prep)


def cdot(ar, ai, br, bi):
    p = dot(
        jnp.concatenate([ar, ai], 0).astype(BF), jnp.concatenate([br, bi], 1).astype(BF)
    )
    rows, cols = ar.shape[0], br.shape[1]
    return p[:rows, :cols] - p[rows:, cols:], p[:rows, cols:] + p[rows:, :cols]


def orth_kernel(x_ref, own_ref, out_ref):
    x = x_ref[...]
    p = dot(x.T, x)
    s_r = p[:256, :256] + p[256:, 256:]
    s_i = p[:256, 256:] - p[256:, :256]
    row = lax.broadcasted_iota(jnp.int32, (256, 256), 0)
    col = lax.broadcasted_iota(jnp.int32, (256, 256), 1)
    eye = (row == col).astype(F32)
    trace = jnp.sum(jnp.sum(s_r * eye, 0, keepdims=True), 1, keepdims=True)
    square = 256 / (2.0 * trace)
    scale = jnp.sqrt(square)
    d_r = 0.5 * (eye - square * s_r)
    d_i = -0.5 * (square * s_i)
    own = own_ref[...]
    y_r, y_i = own[:, :256], own[:, 256:]
    for turn in range(3):
        if turn:
            q_r, q_i = cdot(d_r, d_i, d_r, d_i)
            c_r, c_i = cdot(q_r, q_i, d_r, d_i)
            d_r, d_i = 1.5 * q_r + c_r, 1.5 * q_i + c_i
        e_r, e_i = cdot(y_r, y_i, d_r, d_i)
        y_r, y_i = y_r + e_r, y_i + e_i
    out_ref[:, 0] = scale * y_r
    out_ref[:, 1] = scale * y_i


def orthonormalized(full, own):
    vmem = pl.BlockSpec(memory_space=pltpu.VMEM)
    return pl.pallas_call(
        orth_kernel,
        out_shape=jax.ShapeDtypeStruct((64, 2, 256), F32),
        in_specs=[vmem, vmem],
        out_specs=vmem,
        compiler_params=pltpu.CompilerParams(vmem_limit_bytes=48 << 20),
        name="orthonormalize",
    )(full, own)


def within_half(x):
    return lax.all_to_all(x, "col", 0, 0, tiled=True, axis_index_groups=HALVES)


def partner(x, axis, bit):
    length = lax.axis_size(axis)
    return lax.ppermute(x, axis, [(i, i ^ bit) for i in range(length)])


def half_ring_permutation():
    pairs = []
    for k in range(64):
        for c in range(8):
            pairs.append((8 * k + c, 8 * (k ^ 8) + (c ^ 4)))
    return pairs


def per_device(correlations, gauge, neighbours, shifts):
    kpoint_index = lax.axis_index("ka")
    cindex = lax.axis_index("col")
    near, shift = neighbours[0], shifts[0]

    own = lax.optimization_barrier(gauge[0].reshape(64, 512))
    early = sorted_by_owner(kpoint_index, near, correlations[0], 0, EARLY)
    late = sorted_by_owner(kpoint_index, near, correlations[0], EARLY, 64 - EARLY)
    early = lax.all_to_all(early, "col", 0, 0, tiled=True)
    late = lax.all_to_all(late, "col", 0, 0, tiled=True)
    pair = jnp.stack([own, partner(own, "col", 4)])
    full = jnp.stack([pair, partner(pair, "col", 2)])
    full = jnp.stack([full, partner(full, "col", 1)]).reshape(8, 64, 512)
    near_full = lax.ppermute(full, ("ka", "col"), fetch_permutation())
    outer = jnp.logical_or(cindex == 0, cindex == 7)
    holders = jnp.stack([cindex, jnp.where(outer, 7 - cindex, cindex)])

    owners = owner_of(kpoint_index, *difference(near, kpoint_index))
    weights = shell_vector_weights(kpoint_index, near, shift)
    weight = jnp.sum(jnp.where(owners == cindex, weights, 0.0))

    prep = prepared(holders, early, full, near_full)
    z = main_products(weight, holders, early, late, prep)

    z = within_half(z).astype(F32).sum(0)
    arrived = jnp.concatenate([z[0, :64], z[1]], 0).astype(BF)
    arrived = partner(arrived, "col", 4).astype(F32)
    x = pair.astype(F32) + z[:, :64] + jnp.stack([arrived[64:128], arrived[:64]])
    full_x = x.astype(BF).reshape(128, 512)
    for bit in (2, 1):
        full_x = jnp.concatenate([full_x, partner(full_x, "col", bit)], 0)
    carries = jnp.arange(256)[None] == 32 * cindex
    groups = [[16 * y + 8 * z_hi + x for y in range(4) for x in range(8)] for z_hi in range(2)]
    spread = jnp.broadcast_to(jnp.where(carries, z[0, 64:65, :256], 0.0), (32, 256))
    spread = lax.all_to_all(spread, "ka", 0, 0, tiled=True, axis_index_groups=groups)
    spread = jnp.broadcast_to(spread.sum(0, keepdims=True), (8, 256))
    spread = spread + partner(spread, "col", 4)
    spread = spread + lax.ppermute(spread, ("ka", "col"), half_ring_permutation())
    u_next = orthonormalized(full_x, x[0])
    g = z[0, 64:] + arrived[128:]
    first = jnp.logical_and(carries, jnp.arange(32)[:, None] == 0)
    gradient = jnp.stack([jnp.where(first, 0.0, g[:, :256]), g[:, 256:]])[None]
    return (u_next[None], gradient, jnp.sum(spread[0]))


def solution(mesh):
    return jax.shard_map(
        per_device,
        mesh=mesh,
        in_specs=(
            P("ka", None, None, "col", None),
            P("ka", "col", None, None),
            P("ka", None),
            P("ka", None, None),
        ),
        out_specs=(P("ka", "col", None, None), P("ka", None, "col", None), P()),
        check_vma=False,
    )
```
